128 devices in a mesh: dom: 128 (over y, x, z, core).
Axes of the slice: x: 4, y: 4, z: 4, core: 2. Of those that a mesh axis runs over, the one named last changes fastest.
Arguments:
- start_point: float32 [65536, 128], P('dom'), may hold values from -6 to 6
- residual: float32 [65536, 128], P('dom'), may hold values from -40 to 40
- direction: float32 [65536, 128], P('dom'), may hold values from -40 to 40
- send_list: int32 [128, 4, 3], P('dom'), may hold values from 0 to 3, as said below
- block_cols: int32 [512, 6], P('dom'), may hold values from 0 to 15, as said below
- block_vals: float32 [512, 6, 128, 128], P('dom'), may hold values from -0.2 to 8.1, as said below
Outputs:
- new_point: float32 [65536, 128], P('dom')
- new_residual: float32 [65536, 128], P('dom')
- new_direction: float32 [65536, 128], P('dom')
The draws below stay inside these ranges and needn't reach their ends.
Inputs may be any that keep to these rules, and one draw needn't show every extreme that they name: send_list[t, m] lists, in its first entries, the distinct blocks of partition t that the partition at offset -off (off as in the first step) reads; between 1 and 3 of them are read for each pair, and some pair reads 3; the other entries are valid block numbers that are never read. `block_cols`: entry 0 of a block row names the row's own block; a block that couples two partitions appears in both partitions' rows, transposed; the assembled matrix is symmetric positive definite. `block_vals`: stored blocks that no coupling uses are zero.
All inputs are finite; a program needn't handle non-finite values.
Results may differ from the reference program's by a relative error of at most 0.0003.
Values sent between devices are 32-bit elements; how exact they have to be, the bound alone decides.
A program may use at most 128 MiB of HBM per device.

```python
import math
import jax
import jax.numpy as jnp
from jax import lax

BLOCK = 128
NB = 4
NRHS = 128
HOPS = 2
CAP = 3
STEPS = 6
SLOTS = 6
BASIS = 13
NBLK = 512


def ordering(key, dev_count):
    scores = jax.random.randint(key, (dev_count, NB), 0, 1 << 20) * NB + jnp.arange(NB)[None, :]
    order_ids = jnp.argsort(scores, axis=1).astype(jnp.int32)
    rank_ids = jnp.argsort(order_ids, axis=1).astype(jnp.int32)
    return (order_ids, rank_ids)


def structure(key):
    dev_count = NBLK // NB
    base_key = jax.random.fold_in(key, 4242)
    devices = jnp.arange(dev_count, dtype=jnp.int32)
    hop_data = []
    for hop_index in range(HOPS):
        count_key, chosen_key, left_key, right_key = jax.random.split(jax.random.fold_in(base_key, hop_index), 4)
        counts = jax.random.randint(count_key, (dev_count,), 1, CAP + 1)
        chosen = jax.random.randint(chosen_key, (), 0, dev_count)
        counts = jnp.where(devices == chosen, CAP, counts).astype(jnp.int32)
        left_order, left_rank = ordering(left_key, dev_count)
        right_order, right_rank = ordering(right_key, dev_count)
        hop_data.append((counts, left_order, left_rank, right_order, right_rank))
    local_order, local_rank = ordering(jax.random.fold_in(base_key, 99), dev_count)
    return (hop_data, local_order, local_rank)


def draw_send_list(key, part):
    dev_count = NBLK // NB
    devices = jnp.arange(dev_count, dtype=jnp.int32)
    hop_data, local_order, local_rank = structure(key)
    right_parts = []
    left_parts = []
    for hop_index in range(HOPS):
        counts, left_order, left_rank, right_order, right_rank = hop_data[hop_index]
        distance = hop_index + 1
        right_parts.append(right_order[(devices - distance) % dev_count, :CAP])
        left_parts.append(left_order[:, :CAP])
    return jnp.stack(right_parts + left_parts, axis=1).astype(jnp.int32)


def draw_block_cols(key, part):
    dev_count = NBLK // NB
    devices = jnp.arange(dev_count, dtype=jnp.int32)
    hop_data, local_order, local_rank = structure(key)
    own_blocks = jnp.broadcast_to(jnp.arange(NB, dtype=jnp.int32)[None, :], (dev_count, NB))
    local_partner = jnp.take_along_axis(local_order, jnp.bitwise_xor(local_rank, 1), axis=1)
    plus_cols = []
    minus_cols = []
    for hop_index in range(HOPS):
        counts, left_order, left_rank, right_order, right_rank = hop_data[hop_index]
        distance = hop_index + 1
        is_valid = left_rank < counts[:, None]
        plus_cols.append(jnp.where(is_valid, NB + hop_index * CAP + left_rank, own_blocks))
        left_dev = (devices - distance) % dev_count
        edge_rank = right_rank[left_dev]
        valid_right = edge_rank < counts[left_dev][:, None]
        minus_cols.append(jnp.where(valid_right, NB + (HOPS + hop_index) * CAP + edge_rank, own_blocks))
    joined = jnp.stack([own_blocks, local_partner] + plus_cols + minus_cols, axis=2)
    return joined.reshape(NBLK, SLOTS).astype(jnp.int32)


def draw_block_vals(key, part):
    dev_count = NBLK // NB
    devices = jnp.arange(dev_count, dtype=jnp.int32)
    hop_data, local_order, local_rank = structure(key)
    value_key = jax.random.fold_in(key, 5151)
    diag_key, noise_key, local_key = jax.random.split(value_key, 3)
    diag_vals = jnp.exp(jax.random.uniform(diag_key, (dev_count, NB, BLOCK), minval=math.log(1.6), maxval=math.log(8.0)))
    noise = jax.random.truncated_normal(noise_key, -6.0, 6.0, (dev_count, NB, BLOCK, BLOCK)) * (0.02 / math.sqrt(BLOCK))
    eye_block = jnp.eye(BLOCK, dtype=jnp.float32)
    diag_blocks = eye_block[None, None] * diag_vals[..., None] + 0.5 * (noise + jnp.swapaxes(noise, -1, -2))
    local_table = jax.random.truncated_normal(local_key, -6.0, 6.0, (dev_count, NB // 2, BLOCK, BLOCK)) * (0.15 / math.sqrt(BLOCK))
    pair_ids = local_rank // 2
    is_first = local_rank % 2 == 0
    picked = local_table[devices[:, None], pair_ids]
    local_vals = jnp.where(is_first[..., None, None], picked, jnp.swapaxes(picked, -1, -2))
    plus_vals = []
    minus_vals = []
    for hop_index in range(HOPS):
        counts, left_order, left_rank, right_order, right_rank = hop_data[hop_index]
        distance = hop_index + 1
        coupling = jax.random.truncated_normal(jax.random.fold_in(value_key, 100 + hop_index), -6.0, 6.0, (dev_count, CAP, BLOCK, BLOCK)) * (0.15 / math.sqrt(BLOCK))
        is_valid = (left_rank < counts[:, None]).astype(jnp.float32)
        edge_left = jnp.minimum(left_rank, CAP - 1)
        plus_vals.append(coupling[devices[:, None], edge_left] * is_valid[..., None, None])
        left_dev = (devices - distance) % dev_count
        edge_rank = right_rank[left_dev]
        valid_right = (edge_rank < counts[left_dev][:, None]).astype(jnp.float32)
        edge_right = jnp.minimum(edge_rank, CAP - 1)
        minus_vals.append(jnp.swapaxes(coupling[left_dev[:, None], edge_right], -1, -2) * valid_right[..., None, None])
    joined = jnp.stack([diag_blocks, local_vals] + plus_vals + minus_vals, axis=2)
    return joined.reshape(NBLK, SLOTS, BLOCK, BLOCK).astype(jnp.float32)


def rising_field(key, marker):
    row_count = NBLK * BLOCK
    dev_count = NBLK // NB
    sub_key = jax.random.fold_in(key, marker)
    owner_ids = jnp.arange(row_count) // (NB * BLOCK)
    ramp_vals = 1.0 + 2.0 * owner_ids.astype(jnp.float32) / max(dev_count - 1, 1)
    values = jax.random.truncated_normal(sub_key, -6.0, 6.0, (row_count, NRHS))
    return (values * ramp_vals[:, None]).astype(jnp.float32)


def draw_residual(key, part):
    return rising_field(key, 311)


def draw_direction(key, part):
    return rising_field(key, 733)


def steps_of(rng, dims, pieces, smallest, top_value):
    factor_of, own = 1.0, jax.random.fold_in(rng, 6)
    for position, parts in pieces:
        steps = jnp.exp(jax.random.uniform(jax.random.fold_in(own, position), (parts,), jnp.float32, smallest / len(pieces), top_value / len(pieces)))
        factor_of = factor_of * jnp.repeat(steps, dims[position] // parts).reshape([-1 if axis == position else 1 for axis in range(len(dims))])
    return factor_of


def scatter_about(own_key, dims, deviation, bound, cuts=(), kind=jnp.bfloat16):
    array = deviation * jax.random.normal(own_key, dims, jnp.float32)
    if cuts:
        array = array * steps_of(own_key, dims, cuts, -0.22, 0.18)
    return jnp.clip(array, -bound, bound).astype(kind)


def setup_inputs(seed: int = 0) -> dict:
    key_of = jax.random.split(jax.random.key(seed), 7)
    return {
        "start_point": scatter_about(key_of[0], (NBLK * BLOCK, NRHS), 1.0, 6.0, ((0, 128),), jnp.float32),
        "residual": draw_residual(jax.random.fold_in(key_of[6], 71), 0),
        "direction": draw_direction(jax.random.fold_in(key_of[6], 71), 0),
        "send_list": draw_send_list(jax.random.fold_in(key_of[6], 71), 0),
        "block_cols": draw_block_cols(jax.random.fold_in(key_of[6], 71), 0),
        "block_vals": draw_block_vals(jax.random.fold_in(key_of[6], 71), 0),
    }


center_value = 4.5
half_range = 4.5


def slot_offset(slot_index):
    return slot_index + 1 if slot_index < HOPS else HOPS - 1 - slot_index


def global_columns(block_cols, send_list):
    dev_count = NBLK // NB
    devices = jnp.arange(dev_count, dtype=jnp.int32)
    tables = [devices[:, None] * NB + jnp.arange(NB, dtype=jnp.int32)[None, :]]
    for slot_index in range(2 * HOPS):
        partner = (devices + slot_offset(slot_index)) % dev_count
        tables.append(partner[:, None] * NB + send_list[partner, slot_index, :].astype(jnp.int32))
    joined = jnp.concatenate(tables, axis=1).astype(jnp.int32)
    owners = jnp.arange(NBLK, dtype=jnp.int32) // NB
    return jnp.take_along_axis(joined[owners], block_cols.astype(jnp.int32), axis=1)


def apply_matrix(vector, columns, block_vals):
    blocked = vector.reshape(NBLK, BLOCK, vector.shape[1])
    running = jnp.zeros(blocked.shape, jnp.float32)
    for slot_index in range(SLOTS):
        picked = jnp.take(blocked, columns[:, slot_index], axis=0)
        running = running + jnp.einsum("ibc,icw->ibw", block_vals[:, slot_index], picked, precision=lax.Precision.HIGHEST)
    return running.reshape(vector.shape)


def next_vector(vector, columns, block_vals):
    return (apply_matrix(vector, columns, block_vals) - center_value * vector) / half_range


def basis_change():
    positions = jnp.arange(BASIS)
    row_ids = positions[:, None]
    col_ids = positions[None, :]
    active = (col_ids < STEPS) | ((col_ids > STEPS) & (col_ids < BASIS - 1))
    change_table = jnp.where(active & (row_ids == col_ids), center_value, 0.0)
    change_table = change_table + jnp.where(active & (row_ids == col_ids + 1), half_range, 0.0)
    return change_table.astype(jnp.float32)


def coefficient_steps(gram_matrix):
    change_table = basis_change()
    column_count = gram_matrix.shape[0]
    positions = jnp.arange(BASIS)
    point_c = jnp.zeros((column_count, BASIS), jnp.float32)
    resid_c = jnp.broadcast_to((positions == STEPS + 1).astype(jnp.float32), (column_count, BASIS))
    direc_c = jnp.broadcast_to((positions == 0).astype(jnp.float32), (column_count, BASIS))
    highest = lax.Precision.HIGHEST
    for step_index in range(STEPS):
        current = jnp.sum(resid_c * jnp.einsum("nab,nb->na", gram_matrix, resid_c, precision=highest), axis=1)
        moved_dir = jnp.einsum("ab,nb->na", change_table, direc_c, precision=highest)
        curvature = jnp.sum(direc_c * jnp.einsum("nab,nb->na", gram_matrix, moved_dir, precision=highest), axis=1)
        alpha_step = current / curvature
        point_c = point_c + alpha_step[:, None] * direc_c
        resid_c = resid_c - alpha_step[:, None] * moved_dir
        following = jnp.sum(resid_c * jnp.einsum("nab,nb->na", gram_matrix, resid_c, precision=highest), axis=1)
        direc_c = resid_c + (following / current)[:, None] * direc_c
    return point_c, resid_c, direc_c


def combine_basis(weights, basis_all):
    running = jnp.zeros(basis_all[0].shape, jnp.float32)
    for basis_index in range(BASIS):
        running = running + weights[:, basis_index][None, :] * basis_all[basis_index]
    return running


def reference(start_point, residual, direction, send_list, block_cols, block_vals):
    columns = global_columns(block_cols, send_list)
    p_basis = [direction]
    for power_step in range(STEPS):
        p_basis.append(next_vector(p_basis[-1], columns, block_vals))
    r_basis = [residual]
    for power_step in range(STEPS - 1):
        r_basis.append(next_vector(r_basis[-1], columns, block_vals))
    basis_all = p_basis + r_basis
    gram_matrix = jnp.stack([jnp.stack([jnp.sum(basis_all[first] * basis_all[second], axis=0) for second in range(BASIS)], axis=1) for first in range(BASIS)], axis=1)
    point_c, resid_c, direc_c = coefficient_steps(gram_matrix)
    new_point = start_point + combine_basis(point_c, basis_all)
    new_residual = combine_basis(resid_c, basis_all)
    new_direction = combine_basis(direc_c, basis_all)
    return new_point, new_residual, new_direction
```

```python
import functools

import jax
import jax.numpy as jnp
from jax import lax
from jax.experimental import pallas as pl
from jax.experimental.pallas import tpu as pltpu
from jax.sharding import PartitionSpec as P

MESH = pl.DeviceIdType.MESH
STEPS = 6
BASIS = 13
BLOCK = 128
NB = 4
SLOTS = 6
CAP = 3
OFFSETS = (1, 2, -1, -2)
NEAR = 8
MOMENTS = 40
PP, PR, RR = 0, 13, 24
center_value = 4.5
half_range = 4.5


def split_two(value):
    high = value.astype(jnp.bfloat16)
    low = (value - high.astype(jnp.float32)).astype(jnp.bfloat16)
    return high, low


def kernel(
    peers,
    start_hbm, resid_hbm, direc_hbm, send_ref, cols_ref, vals_hbm,
    point_hbm, newres_hbm, newdir_hbm,
    p_basis, r_basis, start_v, vals_v, mats, diag, table,
    stage_p, stage_r, ghost_p, ghost_r,
    moments, near_buf, near_sum, far_buf, total, late, late_near, late_sum, late_far,
    gram, coefs, outs,
    load_sem, out_sem, send_p, recv_p, send_r, recv_r,
    near_send, near_recv, far_send, far_recv, lnear_send, lnear_recv, lfar_send, lfar_recv,
):
    me = lax.axis_index("dom")
    low = lax.rem(me, NEAR)
    base = me - low
    high = me // NEAR
    far_count = peers // NEAR

    loads = [
        pltpu.make_async_copy(direc_hbm, p_basis.at[0], load_sem.at[0]),
        pltpu.make_async_copy(resid_hbm, r_basis.at[0], load_sem.at[1]),
        pltpu.make_async_copy(vals_hbm, vals_v, load_sem.at[2]),
        pltpu.make_async_copy(start_hbm, start_v, load_sem.at[3]),
    ]
    for load in loads:
        load.start()

    near_peers = [(base + lax.rem(low + d, NEAR), lax.rem(low + d, NEAR)) for d in range(1, NEAR)]
    far_peers = [
        (lax.rem(high + d, far_count) * NEAR + low, lax.rem(high + d, far_count))
        for d in range(1, far_count)
    ]
    barrier = pltpu.get_barrier_semaphore()
    for offset in OFFSETS:
        pl.semaphore_signal(
            barrier, inc=1, device_id=(lax.rem(me - offset + peers, peers),), device_id_type=MESH
        )
    for device, _ in near_peers + far_peers:
        pl.semaphore_signal(barrier, inc=1, device_id=(device,), device_id_type=MESH)
    pl.semaphore_wait(barrier, len(OFFSETS) + len(near_peers) + len(far_peers))

    def exchange(stage, ghost, sends, recvs, parity):
        return [
            pltpu.make_async_remote_copy(
                src_ref=stage.at[m],
                dst_ref=ghost.at[parity, m],
                send_sem=sends.at[m],
                recv_sem=recvs.at[parity, m],
                device_id=(lax.rem(me - offset + peers, peers),),
                device_id_type=MESH,
            )
            for m, offset in enumerate(OFFSETS)
        ]

    def send(basis, step, stage, ghost, sends, recvs):
        copies = exchange(stage, ghost, sends, recvs, lax.rem(step, 2))
        for m in (1, 3, 0, 2):
            for e in range(CAP):
                stage[m, e] = basis[step, send_ref[0, m, e]]
            copies[m].start()

    def own_table(basis, step):
        hi, lo = split_two(basis[step])
        table[0:NB, :, 0:BLOCK] = hi
        table[0:NB, :, BLOCK:] = lo

    def advance(basis, step, stage, ghost, sends, recvs):
        own_table(basis, step)
        parity = lax.rem(step, 2)
        copies = exchange(stage, ghost, sends, recvs, parity)
        for m in (0, 2, 1, 3):
            copies[m].wait_recv()
            hi, lo = split_two(ghost[parity, m])
            at = NB + m * CAP
            table[at : at + CAP, :, 0:BLOCK] = hi
            table[at : at + CAP, :, BLOCK:] = lo
        for copy in copies:
            copy.wait_send()
        for i in range(NB):
            parts = None
            for k in range(0, SLOTS, 2):
                pair = jnp.concatenate([table[cols_ref[i, k]], table[cols_ref[i, k + 1]]], axis=0)
                term = jnp.dot(
                    mats[i, :, k * BLOCK : (k + 2) * BLOCK], pair, preferred_element_type=jnp.float32
                )
                parts = term if parts is None else parts + term
            image = parts[0:BLOCK, 0:BLOCK] + (parts[0:BLOCK, BLOCK:] + parts[BLOCK:, 0:BLOCK])
            basis[step + 1, i] = image + diag[i] * basis[step, i]

    def dot_of(one, two):
        return jnp.sum(jnp.sum((one * two).reshape(-1, 8, BLOCK), axis=0), axis=0, keepdims=True)

    def dots(target, pairs):
        for row, one, two in pairs:
            target[pl.ds(row, 1), :] = dot_of(one, two)

    def level(step):
        p_new, p_old = p_basis[step], p_basis[step - 1]
        r_new, r_old = r_basis[step], r_basis[step - 1]
        dots(
            moments,
            [
                (PP + 2 * step, p_new, p_new),
                (PP + 2 * step - 1, p_new, p_old),
                (PR + 2 * step, p_new, r_new),
                (PR + 2 * step - 1, p_new, r_old),
                (RR + 2 * step, r_new, r_new),
                (RR + 2 * step - 1, r_new, r_old),
            ],
        )

    def group_copy(source, target, sends, recvs, n, device, slot):
        return pltpu.make_async_remote_copy(
            src_ref=source,
            dst_ref=target.at[slot],
            send_sem=sends.at[n],
            recv_sem=recvs.at[slot],
            device_id=(device,),
            device_id_type=MESH,
        )

    def group_start(source, target, sends, recvs, mine, group):
        for n, (device, _) in enumerate(group):
            group_copy(source, target, sends, recvs, n, device, mine).start()

    def group_sum(source, target, sends, recvs, mine, group):
        for n, (device, slot) in enumerate(group):
            group_copy(source, target, sends, recvs, n, device, slot).wait()
        target[mine] = source[...]
        return jnp.sum(target[...], axis=0)

    loads[0].wait()
    send(p_basis, 0, stage_p, ghost_p, send_p, recv_p)
    loads[1].wait()
    send(r_basis, 0, stage_r, ghost_r, send_r, recv_r)
    loads[2].wait()

    rows = lax.broadcasted_iota(jnp.int32, (BLOCK, BLOCK), 0)
    lanes = lax.broadcasted_iota(jnp.int32, (BLOCK, BLOCK), 1)
    for i in range(NB):
        for k in range(SLOTS):
            values = vals_v[i, k]
            if k == 0:
                on_diag = jnp.where(rows == lanes, values, 0.0)
                column = (jnp.sum(on_diag, axis=1, keepdims=True) - center_value) / half_range
                diag[i] = jnp.broadcast_to(column, (BLOCK, BLOCK))
                values = jnp.where(rows == lanes, 0.0, values)
            hi, lo = split_two(values * (1.0 / half_range))
            mats[i, 0:BLOCK, k * BLOCK : (k + 1) * BLOCK] = hi
            mats[i, BLOCK:, k * BLOCK : (k + 1) * BLOCK] = lo
    moments[...] = jnp.zeros_like(moments)
    late[...] = jnp.zeros_like(late)
    gram[...] = jnp.zeros_like(gram)
    dots(
        moments,
        [
            (PP, p_basis[0], p_basis[0]),
            (PR, p_basis[0], r_basis[0]),
            (RR, r_basis[0], r_basis[0]),
        ],
    )

    def step_body(step, carry):
        advance(p_basis, step, stage_p, ghost_p, send_p, recv_p)
        send(p_basis, step + 1, stage_p, ghost_p, send_p, recv_p)
        advance(r_basis, step, stage_r, ghost_r, send_r, recv_r)

        @pl.when(step < STEPS - 2)
        def _():
            send(r_basis, step + 1, stage_r, ghost_r, send_r, recv_r)

        level(step + 1)
        return carry

    lax.fori_loop(0, STEPS - 1, step_body, 0)

    group_start(moments, near_buf, near_send, near_recv, low, near_peers)
    near_sum[...] = group_sum(moments, near_buf, near_send, near_recv, low, near_peers)
    group_start(near_sum, far_buf, far_send, far_recv, high, far_peers)

    advance(p_basis, STEPS - 1, stage_p, ghost_p, send_p, recv_p)
    p_last = p_basis[STEPS]
    dots(
        late,
        [
            (0, p_last, p_basis[STEPS - 1]),
            (1, p_last, p_last),
            (2, p_last, r_basis[STEPS - 1]),
        ],
    )
    group_start(late, late_near, lnear_send, lnear_recv, low, near_peers)
    late_sum[...] = group_sum(late, late_near, lnear_send, lnear_recv, low, near_peers)
    group_start(late_sum, late_far, lfar_send, lfar_recv, high, far_peers)
    loads[3].wait()
    total[...] = group_sum(near_sum, far_buf, far_send, far_recv, high, far_peers)
    last = group_sum(late_sum, late_far, lfar_send, lfar_recv, high, far_peers)
    total[PP + 11 : PP + 13, :] = last[0:2]
    pr_last = last[2:3]

    def pr_rows(first, count):
        wanted = min(first + count, 11) - first
        part = total[PR + first : PR + first + wanted, :]
        return part if wanted == count else jnp.concatenate([part, pr_last], axis=0)

    for b in range(STEPS + 1):
        gram[b, 0 : STEPS + 1, :] = total[PP + b : PP + b + STEPS + 1, :]
        gram[b, STEPS + 1 : BASIS, :] = pr_rows(b, STEPS)
    for b in range(STEPS):
        gram[STEPS + 1 + b, 0 : STEPS + 1, :] = pr_rows(b, STEPS + 1)
        gram[STEPS + 1 + b, STEPS + 1 : BASIS, :] = total[RR + b : RR + b + STEPS, :]

    places = lax.broadcasted_iota(jnp.int32, (16, BLOCK), 0)
    active = (places < STEPS) | ((places > STEPS) & (places < BASIS - 1))

    def times_gram(vector):
        sums = [gram[b] * vector[b : b + 1, :] for b in range(BASIS)]
        while len(sums) > 1:
            sums = [a + b for a, b in zip(sums[::2], sums[1::2])] + (
                [sums[-1]] if len(sums) % 2 else []
            )
        return sums[0]

    def inner(one, two):
        return jnp.sum(one * two, axis=0, keepdims=True)

    point_c = jnp.zeros((16, BLOCK), jnp.float32)
    resid_c = jnp.where(places == STEPS + 1, 1.0, 0.0).astype(jnp.float32)
    direc_c = jnp.where(places == 0, 1.0, 0.0).astype(jnp.float32)
    current = inner(resid_c, times_gram(resid_c))
    for _ in range(STEPS):
        held = jnp.where(active, direc_c, 0.0)
        shifted = jnp.concatenate([jnp.zeros((1, BLOCK), jnp.float32), held[0:15]], axis=0)
        moved = center_value * held + half_range * shifted
        alpha = current / inner(direc_c, times_gram(moved))
        point_c = point_c + alpha * direc_c
        resid_c = resid_c - alpha * moved
        following = inner(resid_c, times_gram(resid_c))
        direc_c = resid_c + (following / current) * direc_c
        current = following
    coefs[0] = point_c
    coefs[1] = resid_c
    coefs[2] = direc_c

    copies = []
    for i in range(NB):
        def combine(chunk, carry):
            at = pl.ds(chunk * 32, 32)
            sums = [start_v[i, at, :], None, None]
            for a in range(BASIS):
                piece = p_basis[a, i, at, :] if a <= STEPS else r_basis[a - STEPS - 1, i, at, :]
                for o in range(3):
                    term = coefs[o, a : a + 1, :] * piece
                    sums[o] = term if sums[o] is None else sums[o] + term
            for o in range(3):
                outs[o, i, at, :] = sums[o]
            return carry

        lax.fori_loop(0, BLOCK // 32, combine, 0)
        for o, target in enumerate((point_hbm, newres_hbm, newdir_hbm)):
            copy = pltpu.make_async_copy(outs.at[o, i], target.at[i], out_sem.at[o, i])
            copy.start()
            copies.append(copy)
    for copy in copies:
        copy.wait()


def shards(start_point, residual, direction, send_list, block_cols, block_vals, *, peers):
    far_count = peers // NEAR
    blocked = (NB, BLOCK, BLOCK)
    any_space = pl.BlockSpec(memory_space=pl.ANY)
    scalars = pl.BlockSpec(memory_space=pltpu.SMEM)
    f32 = jnp.float32
    dma = pltpu.SemaphoreType.DMA
    results = pl.pallas_call(
        functools.partial(kernel, peers),
        out_shape=[jax.ShapeDtypeStruct(blocked, f32)] * 3,
        in_specs=[any_space, any_space, any_space, scalars, scalars, any_space],
        out_specs=[any_space] * 3,
        scratch_shapes=[
            pltpu.VMEM((STEPS + 1, *blocked), f32),
            pltpu.VMEM((STEPS, *blocked), f32),
            pltpu.VMEM(blocked, f32),
            pltpu.VMEM((NB, SLOTS, BLOCK, BLOCK), f32),
            pltpu.VMEM((NB, 2 * BLOCK, SLOTS * BLOCK), jnp.bfloat16),
            pltpu.VMEM(blocked, f32),
            pltpu.VMEM((NB + 4 * CAP, BLOCK, 2 * BLOCK), jnp.bfloat16),
            pltpu.VMEM((4, CAP, BLOCK, BLOCK), f32),
            pltpu.VMEM((4, CAP, BLOCK, BLOCK), f32),
            pltpu.VMEM((2, 4, CAP, BLOCK, BLOCK), f32),
            pltpu.VMEM((2, 4, CAP, BLOCK, BLOCK), f32),
            pltpu.VMEM((MOMENTS, BLOCK), f32),
            pltpu.VMEM((NEAR, MOMENTS, BLOCK), f32),
            pltpu.VMEM((MOMENTS, BLOCK), f32),
            pltpu.VMEM((far_count, MOMENTS, BLOCK), f32),
            pltpu.VMEM((MOMENTS, BLOCK), f32),
            pltpu.VMEM((8, BLOCK), f32),
            pltpu.VMEM((NEAR, 8, BLOCK), f32),
            pltpu.VMEM((8, BLOCK), f32),
            pltpu.VMEM((far_count, 8, BLOCK), f32),
            pltpu.VMEM((BASIS, 16, BLOCK), f32),
            pltpu.VMEM((3, 16, BLOCK), f32),
            pltpu.VMEM((3, *blocked), f32),
            dma((4,)),
            dma((3, NB)),
            dma((4,)),
            dma((2, 4)),
            dma((4,)),
            dma((2, 4)),
            dma((NEAR - 1,)),
            dma((NEAR,)),
            dma((far_count - 1,)),
            dma((far_count,)),
            dma((NEAR - 1,)),
            dma((NEAR,)),
            dma((far_count - 1,)),
            dma((far_count,)),
        ],
        compiler_params=pltpu.CompilerParams(
            collective_id=0, has_side_effects=True, vmem_limit_bytes=56 * 1024 * 1024
        ),
        name="cg_steps",
    )(
        start_point.reshape(blocked),
        residual.reshape(blocked),
        direction.reshape(blocked),
        send_list,
        block_cols,
        block_vals,
    )
    return tuple(result.reshape(NB * BLOCK, BLOCK) for result in results)


def solution(mesh):
    return jax.shard_map(
        functools.partial(shards, peers=mesh.shape["dom"]),
        mesh=mesh,
        in_specs=(
            P("dom", None),
            P("dom", None),
            P("dom", None),
            P("dom", None, None),
            P("dom", None),
            P("dom", None, None, None),
        ),
        out_specs=(P("dom", None), P("dom", None), P("dom", None)),
        check_vma=False,
    )
```

```python
import functools

import jax
import jax.numpy as jnp
from jax import lax
from jax.experimental import pallas as pl
from jax.experimental.pallas import tpu as pltpu
from jax.sharding import PartitionSpec as P

MESH = pl.DeviceIdType.MESH
STEPS = 6
BASIS = 13
BLOCK = 128
NB = 4
SLOTS = 6
CAP = 3
GHOSTS = 14
X_AT, Y_AT, FAR_AT, SIB_AT = 0, 4, 8, 11
NEAR = 8
MOMENTS = 40
VMEM_GRANT = 24 * 1024 * 1024
PP, PR, RR = 0, 13, 24
center_value = 4.5
half_range = 4.5


def split_two(value):
    high = value.astype(jnp.bfloat16)
    low = (value - high.astype(jnp.float32)).astype(jnp.bfloat16)
    return high, low


def kernel(
    peers,
    start_hbm, resid_hbm, direc_hbm, send_hbm, cols_hbm, vals_hbm,
    outs,
    p_basis, r_basis, start_v, vals_v, mats, diag, table,
    stage_p, stage_r, ghost_p, ghost_r,
    moments, near_buf, near_sum, far_buf, total, late, late_near, late_sum, late_far,
    gram, coefs, cols_ref, send_ref, send_vmem, lists_v, lists_s, ghost_map, places,
    load_sem, list_send, list_recv, send_p, recv_p, send_r, recv_r,
    near_send, near_recv, far_send, far_recv, lnear_send, lnear_recv, lfar_send, lfar_recv,
):
    me = lax.axis_index("dom")
    low = lax.rem(me, NEAR)
    base = me - low
    high = me // NEAR
    far_count = peers // NEAR

    odd = lax.rem(me, 2)
    sign = 2 * odd - 1
    x_dev = lax.rem(me + sign + peers, peers)
    y_dev = lax.rem(me - 2 * sign + peers, peers)
    w_dev = lax.rem(me + 2 * sign + peers, peers)
    sibling = me - sign

    loads = [
        pltpu.make_async_copy(direc_hbm, p_basis.at[0], load_sem.at[0]),
        pltpu.make_async_copy(resid_hbm, r_basis.at[0], load_sem.at[1]),
        pltpu.make_async_copy(vals_hbm, vals_v, load_sem.at[2]),
        pltpu.make_async_copy(start_hbm, start_v, load_sem.at[3]),
    ]
    lists = [
        pltpu.make_async_copy(send_hbm, send_ref, load_sem.at[4]),
        pltpu.make_async_copy(send_hbm, send_vmem, load_sem.at[5]),
        pltpu.make_async_copy(cols_hbm, cols_ref, load_sem.at[7]),
    ]
    for load in lists + loads:
        load.start()

    near_peers = [(base + lax.rem(low + d, NEAR), lax.rem(low + d, NEAR)) for d in range(1, NEAR)]
    far_peers = [
        (lax.rem(high + d, far_count) * NEAR + low, lax.rem(high + d, far_count))
        for d in range(1, far_count)
    ]
    barrier = pltpu.get_barrier_semaphore()
    for device in (x_dev, y_dev, w_dev, sibling):
        pl.semaphore_signal(barrier, inc=1, device_id=(device,), device_id_type=MESH)
    for device, _ in near_peers + far_peers:
        pl.semaphore_signal(barrier, inc=1, device_id=(device,), device_id_type=MESH)

    def remote(source, ghost, sends, recvs, parity, at, count, n, device):
        return pltpu.make_async_remote_copy(
            src_ref=source,
            dst_ref=ghost.at[parity, pl.ds(at, count)],
            send_sem=sends.at[n],
            recv_sem=recvs.at[parity, n],
            device_id=(device,),
            device_id_type=MESH,
        )

    def direct(basis, step, stage, ghost, sends, recvs):
        common = (ghost, sends, recvs, lax.rem(step, 2))
        return [
            remote(basis.at[step, pl.ds(2, 2)], *common, X_AT + 2, 2, 0, x_dev),
            remote(basis.at[step, pl.ds(0, 2)], *common, Y_AT, 2, 1, w_dev),
            remote(stage.at[0], *common, FAR_AT, CAP, 2, y_dev),
            remote(stage.at[1], *common, SIB_AT, CAP, 3, sibling),
        ]

    def handed(ghost, sends, recvs, parity):
        common = (ghost, sends, recvs, parity)
        return [
            remote(ghost.at[parity, pl.ds(X_AT + 2, 2)], *common, Y_AT + 2, 2, 5, sibling),
            remote(ghost.at[parity, pl.ds(Y_AT, 2)], *common, X_AT, 2, 4, sibling),
        ]

    far_slot = 3 - 2 * odd
    sib_slot = 2 - 2 * odd

    def fill(basis, step, stage, side):
        for e in range(CAP):
            stage[side, e] = basis[step, send_ref[e, 0, (far_slot, sib_slot)[side]]]

    def send(basis, step, stage, ghost, sends, recvs, filled=False):
        copies = direct(basis, step, stage, ghost, sends, recvs)
        copies[1].start()
        copies[0].start()
        for side in range(2):
            if not filled:
                fill(basis, step, stage, side)
            copies[2 + side].start()

    def own_table(basis, step):
        hi, lo = split_two(basis[step])
        table[0:NB, :, 0:BLOCK] = hi
        table[0:NB, :, BLOCK:] = lo

    def advance(basis, step, stage, ghost, sends, recvs):
        parity = lax.rem(step, 2)
        copies = direct(basis, step, stage, ghost, sends, recvs)
        relays = handed(ghost, sends, recvs, parity)

        def take(at, count):
            hi, lo = split_two(ghost[parity, at : at + count])
            table[NB + at : NB + at + count, :, 0:BLOCK] = hi
            table[NB + at : NB + at + count, :, BLOCK:] = lo

        own_table(basis, step)
        copies[1].wait_recv()
        relays[1].start()
        copies[0].wait_recv()
        relays[0].start()
        copies[3].wait_recv()
        take(SIB_AT, CAP)
        take(Y_AT, 2)
        take(X_AT + 2, 2)
        copies[2].wait_recv()
        take(FAR_AT, CAP)
        relays[1].wait_recv()
        take(X_AT, 2)
        relays[0].wait_recv()
        take(Y_AT + 2, 2)
        for copy in copies + relays:
            copy.wait_send()
        for i in range(NB):
            parts = None
            for k in range(0, SLOTS, 2):
                pair = jnp.concatenate(
                    [table[places[i * SLOTS + k]], table[places[i * SLOTS + k + 1]]], axis=0
                )
                term = jnp.dot(
                    mats[i, :, k * BLOCK : (k + 2) * BLOCK], pair, preferred_element_type=jnp.float32
                )
                parts = term if parts is None else parts + term
            image = parts[0:BLOCK, 0:BLOCK] + (parts[0:BLOCK, BLOCK:] + parts[BLOCK:, 0:BLOCK])
            basis[step + 1, i] = image + diag[i] * basis[step, i]

    def dot_of(one, two):
        return jnp.sum(jnp.sum((one * two).reshape(-1, 8, BLOCK), axis=0), axis=0, keepdims=True)

    def dots(target, pairs):
        for row, one, two in pairs:
            target[pl.ds(row, 1), :] = dot_of(one, two)

    def level(step):
        p_new, p_old = p_basis[step], p_basis[step - 1]
        r_new, r_old = r_basis[step], r_basis[step - 1]
        dots(
            moments,
            [
                (PP + 2 * step, p_new, p_new),
                (PP + 2 * step - 1, p_new, p_old),
                (PR + 2 * step, p_new, r_new),
                (PR + 2 * step - 1, p_new, r_old),
                (RR + 2 * step, r_new, r_new),
                (RR + 2 * step - 1, r_new, r_old),
            ],
        )

    def group_copy(source, target, sends, recvs, n, device, slot):
        return pltpu.make_async_remote_copy(
            src_ref=source,
            dst_ref=target.at[slot],
            send_sem=sends.at[n],
            recv_sem=recvs.at[slot],
            device_id=(device,),
            device_id_type=MESH,
        )

    def group_start(source, target, sends, recvs, mine, group):
        for n, (device, _) in enumerate(group):
            group_copy(source, target, sends, recvs, n, device, mine).start()

    def group_sum(source, target, sends, recvs, mine, group):
        for n, (device, slot) in enumerate(group):
            group_copy(source, target, sends, recvs, n, device, slot).wait()
        target[mine] = source[...]
        return jnp.sum(target[...], axis=0)

    def list_copy(n, device):
        return pltpu.make_async_remote_copy(
            src_ref=send_vmem,
            dst_ref=lists_v.at[n],
            send_sem=list_send.at[n],
            recv_sem=list_recv.at[n],
            device_id=(device,),
            device_id_type=MESH,
        )

    for load in lists + loads[0:2]:
        load.wait()
    for side in range(2):
        fill(p_basis, 0, stage_p, side)
        fill(r_basis, 0, stage_r, side)
    pl.semaphore_wait(barrier, 4 + len(near_peers) + len(far_peers))
    list_copies = [list_copy(0, x_dev), list_copy(1, w_dev)]
    for copy in list_copies:
        copy.start()
    send(p_basis, 0, stage_p, ghost_p, send_p, recv_p, filled=True)
    send(r_basis, 0, stage_r, ghost_r, send_r, recv_r, filled=True)
    loads[2].wait()

    rows = lax.broadcasted_iota(jnp.int32, (BLOCK, BLOCK), 0)
    lanes = lax.broadcasted_iota(jnp.int32, (BLOCK, BLOCK), 1)
    for i in range(NB):
        for k in range(SLOTS):
            values = vals_v[i, k]
            if k == 0:
                on_diag = jnp.where(rows == lanes, values, 0.0)
                column = (jnp.sum(on_diag, axis=1, keepdims=True) - center_value) / half_range
                diag[i] = jnp.broadcast_to(column, (BLOCK, BLOCK))
                values = jnp.where(rows == lanes, 0.0, values)
            hi, lo = split_two(values * (1.0 / half_range))
            mats[i, 0:BLOCK, k * BLOCK : (k + 1) * BLOCK] = hi
            mats[i, BLOCK:, k * BLOCK : (k + 1) * BLOCK] = lo
    moments[...] = jnp.zeros_like(moments)
    late[...] = jnp.zeros_like(late)
    gram[...] = jnp.zeros_like(gram)
    dots(
        moments,
        [
            (PP, p_basis[0], p_basis[0]),
            (PR, p_basis[0], r_basis[0]),
            (RR, r_basis[0], r_basis[0]),
        ],
    )

    for copy in list_copies:
        copy.wait()
    to_scalars = pltpu.make_async_copy(lists_v, lists_s, load_sem.at[6])
    to_scalars.start()
    to_scalars.wait()
    x_slot, y_slot = 2 - 2 * odd, 1 + 2 * odd
    for c in range(NB):
        ghost_map[c] = c
    for e in range(CAP):
        ghost_map[NB + CAP * x_slot + e] = NB + X_AT + lists_s[0, e, 0, x_slot]
        ghost_map[NB + CAP * y_slot + e] = NB + Y_AT + lists_s[1, e, 0, y_slot]
        ghost_map[NB + CAP * (3 - 2 * odd) + e] = NB + FAR_AT + e
        ghost_map[NB + CAP * (2 * odd) + e] = NB + SIB_AT + e
    for i in range(NB):
        for k in range(SLOTS):
            places[i * SLOTS + k] = ghost_map[cols_ref[i, k]]

    def step_body(step, carry):
        advance(p_basis, step, stage_p, ghost_p, send_p, recv_p)
        send(p_basis, step + 1, stage_p, ghost_p, send_p, recv_p)
        advance(r_basis, step, stage_r, ghost_r, send_r, recv_r)

        @pl.when(step < STEPS - 2)
        def _():
            send(r_basis, step + 1, stage_r, ghost_r, send_r, recv_r)

        level(step + 1)
        return carry

    lax.fori_loop(0, STEPS - 1, step_body, 0)

    group_start(moments, near_buf, near_send, near_recv, low, near_peers)
    advance(p_basis, STEPS - 1, stage_p, ghost_p, send_p, recv_p)
    p_last = p_basis[STEPS]
    dots(
        late,
        [
            (0, p_last, p_basis[STEPS - 1]),
            (1, p_last, p_last),
            (2, p_last, r_basis[STEPS - 1]),
        ],
    )
    group_start(late, late_near, lnear_send, lnear_recv, low, near_peers)
    near_sum[...] = group_sum(moments, near_buf, near_send, near_recv, low, near_peers)
    group_start(near_sum, far_buf, far_send, far_recv, high, far_peers)
    late_sum[...] = group_sum(late, late_near, lnear_send, lnear_recv, low, near_peers)
    group_start(late_sum, late_far, lfar_send, lfar_recv, high, far_peers)
    loads[3].wait()
    total[...] = group_sum(near_sum, far_buf, far_send, far_recv, high, far_peers)
    last = group_sum(late_sum, late_far, lfar_send, lfar_recv, high, far_peers)
    total[PP + 11 : PP + 13, :] = last[0:2]
    pr_last = last[2:3]

    def pr_rows(first, count):
        wanted = min(first + count, 11) - first
        part = total[PR + first : PR + first + wanted, :]
        return part if wanted == count else jnp.concatenate([part, pr_last], axis=0)

    for b in range(STEPS + 1):
        gram[b, 0 : STEPS + 1, :] = total[PP + b : PP + b + STEPS + 1, :]
        gram[b, STEPS + 1 : BASIS, :] = pr_rows(b, STEPS)
    for b in range(STEPS):
        gram[STEPS + 1 + b, 0 : STEPS + 1, :] = pr_rows(b, STEPS + 1)
        gram[STEPS + 1 + b, STEPS + 1 : BASIS, :] = total[RR + b : RR + b + STEPS, :]

    places = lax.broadcasted_iota(jnp.int32, (16, BLOCK), 0)
    active = (places < STEPS) | ((places > STEPS) & (places < BASIS - 1))

    def times_gram(vector):
        sums = [gram[b] * vector[b : b + 1, :] for b in range(BASIS)]
        while len(sums) > 1:
            sums = [a + b for a, b in zip(sums[::2], sums[1::2])] + (
                [sums[-1]] if len(sums) % 2 else []
            )
        return sums[0]

    def inner(one, two):
        return jnp.sum(one * two, axis=0, keepdims=True)

    point_c = jnp.zeros((16, BLOCK), jnp.float32)
    resid_c = jnp.where(places == STEPS + 1, 1.0, 0.0).astype(jnp.float32)
    direc_c = jnp.where(places == 0, 1.0, 0.0).astype(jnp.float32)
    current = inner(resid_c, times_gram(resid_c))
    for _ in range(STEPS):
        held = jnp.where(active, direc_c, 0.0)
        shifted = jnp.concatenate([jnp.zeros((1, BLOCK), jnp.float32), held[0:15]], axis=0)
        moved = center_value * held + half_range * shifted
        alpha = current / inner(direc_c, times_gram(moved))
        point_c = point_c + alpha * direc_c
        resid_c = resid_c - alpha * moved
        following = inner(resid_c, times_gram(resid_c))
        direc_c = resid_c + (following / current) * direc_c
        current = following
    coefs[0] = point_c
    coefs[1] = resid_c
    coefs[2] = direc_c

    for i in range(NB):
        def combine(chunk, carry):
            at = pl.ds(chunk * 32, 32)
            sums = [start_v[i, at, :], None, None]
            for a in range(BASIS):
                piece = p_basis[a, i, at, :] if a <= STEPS else r_basis[a - STEPS - 1, i, at, :]
                for o in range(3):
                    term = coefs[o, a : a + 1, :] * piece
                    sums[o] = term if sums[o] is None else sums[o] + term
            for o in range(3):
                outs[o, i, at, :] = sums[o]
            return carry

        lax.fori_loop(0, BLOCK // 32, combine, 0)


def deliver(outs, point_hbm, newres_hbm, newdir_hbm, sems):
    copies = [
        pltpu.make_async_copy(outs.at[o], target, sems.at[o])
        for o, target in enumerate((point_hbm, newres_hbm, newdir_hbm))
    ]
    for copy in copies:
        copy.start()
    for copy in copies:
        copy.wait()


def shards(start_point, residual, direction, send_list, block_cols, block_vals, *, peers):
    far_count = peers // NEAR
    blocked = (NB, BLOCK, BLOCK)
    any_space = pl.BlockSpec(memory_space=pl.ANY)
    f32 = jnp.float32
    in_place = functools.partial(pltpu.with_memory_space_constraint, memory_space=pltpu.HBM)
    dma = pltpu.SemaphoreType.DMA
    outs = pl.pallas_call(
        functools.partial(kernel, peers),
        out_shape=jax.ShapeDtypeStruct((3, *blocked), f32),
        in_specs=[any_space] * 6,
        out_specs=pl.BlockSpec(memory_space=pltpu.VMEM),
        scratch_shapes=[
            pltpu.VMEM((STEPS + 1, *blocked), f32),
            pltpu.VMEM((STEPS, *blocked), f32),
            pltpu.VMEM(blocked, f32),
            pltpu.VMEM((NB, SLOTS, BLOCK, BLOCK), f32),
            pltpu.VMEM((NB, 2 * BLOCK, SLOTS * BLOCK), jnp.bfloat16),
            pltpu.VMEM(blocked, f32),
            pltpu.VMEM((NB + GHOSTS, BLOCK, 2 * BLOCK), jnp.bfloat16),
            pltpu.VMEM((2, CAP, BLOCK, BLOCK), f32),
            pltpu.VMEM((2, CAP, BLOCK, BLOCK), f32),
            pltpu.VMEM((2, GHOSTS, BLOCK, BLOCK), f32),
            pltpu.VMEM((2, GHOSTS, BLOCK, BLOCK), f32),
            pltpu.VMEM((MOMENTS, BLOCK), f32),
            pltpu.VMEM((NEAR, MOMENTS, BLOCK), f32),
            pltpu.VMEM((MOMENTS, BLOCK), f32),
            pltpu.VMEM((far_count, MOMENTS, BLOCK), f32),
            pltpu.VMEM((MOMENTS, BLOCK), f32),
            pltpu.VMEM((8, BLOCK), f32),
            pltpu.VMEM((NEAR, 8, BLOCK), f32),
            pltpu.VMEM((8, BLOCK), f32),
            pltpu.VMEM((far_count, 8, BLOCK), f32),
            pltpu.VMEM((BASIS, 16, BLOCK), f32),
            pltpu.VMEM((3, 16, BLOCK), f32),
            pltpu.SMEM((NB, SLOTS), jnp.int32),
            pltpu.SMEM((CAP, 1, 4), jnp.int32),
            pltpu.VMEM((CAP, 1, 4), jnp.int32),
            pltpu.VMEM((2, CAP, 1, 4), jnp.int32),
            pltpu.SMEM((2, CAP, 1, 4), jnp.int32),
            pltpu.SMEM((NB + 4 * CAP,), jnp.int32),
            pltpu.SMEM((NB * SLOTS,), jnp.int32),
            dma((8,)),
            dma((2,)),
            dma((2,)),
            dma((6,)),
            dma((2, 6)),
            dma((6,)),
            dma((2, 6)),
            dma((NEAR - 1,)),
            dma((NEAR,)),
            dma((far_count - 1,)),
            dma((far_count,)),
            dma((NEAR - 1,)),
            dma((NEAR,)),
            dma((far_count - 1,)),
            dma((far_count,)),
        ],
        compiler_params=pltpu.CompilerParams(
            collective_id=0, has_side_effects=True, vmem_limit_bytes=VMEM_GRANT
        ),
        name="cg_steps",
    )(
        in_place(start_point.reshape(blocked)),
        in_place(residual.reshape(blocked)),
        in_place(direction.reshape(blocked)),
        in_place(jnp.transpose(send_list, (2, 0, 1))),
        in_place(block_cols),
        in_place(block_vals),
    )
    results = pl.pallas_call(
        deliver,
        out_shape=[jax.ShapeDtypeStruct(blocked, f32)] * 3,
        in_specs=[pl.BlockSpec(memory_space=pltpu.VMEM)],
        out_specs=[any_space] * 3,
        scratch_shapes=[dma((3,))],
        compiler_params=pltpu.CompilerParams(vmem_limit_bytes=4 * 1024 * 1024),
        name="deliver",
    )(outs)
    return tuple(result.reshape(NB * BLOCK, BLOCK) for result in results)


def solution(mesh):
    return jax.shard_map(
        functools.partial(shards, peers=mesh.shape["dom"]),
        mesh=mesh,
        in_specs=(
            P("dom", None),
            P("dom", None),
            P("dom", None),
            P("dom", None, None),
            P("dom", None),
            P("dom", None, None, None),
        ),
        out_specs=(P("dom", None), P("dom", None), P("dom", None)),
        check_vma=False,
    )
```

```python
import functools

import jax
import jax.numpy as jnp
from jax import lax
from jax.experimental import pallas as pl
from jax.experimental.pallas import tpu as pltpu
from jax.sharding import PartitionSpec as P

MESH = pl.DeviceIdType.MESH
STEPS = 6
BASIS = 13
BLOCK = 128
NB = 4
SLOTS = 6
CAP = 3
GHOSTS = 14
X_AT, Y_AT, FAR_AT, SIB_AT = 0, 4, 8, 11
NEAR = 8
MOMENTS = 40
VMEM_GRANT = 24 * 1024 * 1024
PP, PR, RR = 0, 13, 24
center_value = 4.5
half_range = 4.5


def split_two(value):
    high = value.astype(jnp.bfloat16)
    low = (value - high.astype(jnp.float32)).astype(jnp.bfloat16)
    return high, low


def kernel(
    peers,
    start_hbm, resid_hbm, direc_hbm, send_hbm, cols_hbm, vals_hbm,
    outs,
    p_basis, r_basis, start_v, vals_v, mats, diag, table,
    stage_p, stage_r, ghost_p, ghost_r, hand_p, hand_r,
    moments, near_buf, near_sum, far_buf, total, late, late_near, late_sum, late_far,
    gram, coefs, cols_ref, send_ref, send_vmem, lists_v, lists_s, ghost_map, places,
    load_sem, list_send, list_recv, send_p, recv_p, send_r, recv_r,
    near_send, near_recv, far_send, far_recv, lnear_send, lnear_recv, lfar_send, lfar_recv,
):
    me = lax.axis_index("dom")
    low = lax.rem(me, NEAR)
    base = me - low
    high = me // NEAR
    far_count = peers // NEAR

    odd = lax.rem(me, 2)
    sign = 2 * odd - 1
    x_dev = lax.rem(me + sign + peers, peers)
    y_dev = lax.rem(me - 2 * sign + peers, peers)
    w_dev = lax.rem(me + 2 * sign + peers, peers)
    sibling = me - sign

    loads = [
        pltpu.make_async_copy(direc_hbm, p_basis.at[0], load_sem.at[0]),
        pltpu.make_async_copy(resid_hbm, r_basis.at[0], load_sem.at[1]),
        pltpu.make_async_copy(vals_hbm, vals_v, load_sem.at[2]),
        pltpu.make_async_copy(start_hbm, start_v, load_sem.at[3]),
    ]
    lists = [
        pltpu.make_async_copy(send_hbm, send_ref, load_sem.at[4]),
        pltpu.make_async_copy(send_hbm, send_vmem, load_sem.at[5]),
        pltpu.make_async_copy(cols_hbm, cols_ref, load_sem.at[7]),
    ]
    for load in lists + loads:
        load.start()

    near_peers = [(base + lax.rem(low + d, NEAR), lax.rem(low + d, NEAR)) for d in range(1, NEAR)]
    far_peers = [
        (lax.rem(high + d, far_count) * NEAR + low, lax.rem(high + d, far_count))
        for d in range(1, far_count)
    ]
    barrier = pltpu.get_barrier_semaphore()
    for device in (x_dev, y_dev, w_dev, sibling):
        pl.semaphore_signal(barrier, inc=1, device_id=(device,), device_id_type=MESH)
    for device, _ in near_peers + far_peers:
        pl.semaphore_signal(barrier, inc=1, device_id=(device,), device_id_type=MESH)

    def remote(source, target, sends, recvs, parity, n, device):
        return pltpu.make_async_remote_copy(
            src_ref=source,
            dst_ref=target,
            send_sem=sends.at[n],
            recv_sem=recvs.at[parity, n],
            device_id=(device,),
            device_id_type=MESH,
        )

    def copies_of(chain, step):
        basis, stage, ghost, hand, sends, recvs = chain
        parity = lax.rem(step, 2)

        def part(at, count):
            return ghost.at[parity, pl.ds(at, count)]

        def to(n, source, target, device):
            return remote(source, target, sends, recvs, parity, n, device)

        return dict(
            upper=to(0, basis.at[step, pl.ds(2, 2)], part(X_AT + 2, 2), x_dev),
            lower=to(1, basis.at[step, pl.ds(0, 2)], part(Y_AT, 2), w_dev),
            onward=to(2, hand.at[parity], part(FAR_AT, CAP), x_dev),
            beside=to(3, stage.at[1], part(SIB_AT, CAP), sibling),
            relay_y=to(4, part(Y_AT, 2), part(X_AT, 2), sibling),
            relay_x=to(5, part(X_AT + 2, 2), part(Y_AT + 2, 2), sibling),
            over=to(6, stage.at[0], hand.at[parity], sibling),
        )

    far_slot = 3 - 2 * odd
    sib_slot = 2 - 2 * odd

    def fill(chain, step, side):
        basis, stage = chain[0:2]
        for e in range(CAP):
            stage[side, e] = basis[step, send_ref[e, 0, (far_slot, sib_slot)[side]]]

    def send_rest(chain, step, filled=False):
        copies = copies_of(chain, step)
        copies["upper"].start()
        for side, name in enumerate(("over", "beside")):
            if not filled:
                fill(chain, step, side)
            copies[name].start()

    def forward(chain, step):
        copies = copies_of(chain, step)
        copies["over"].wait_recv()
        copies["onward"].start()

    def own_table(chain, step):
        hi, lo = split_two(chain[0][step])
        table[0:NB, :, 0:BLOCK] = hi
        table[0:NB, :, BLOCK:] = lo

    def advance(chain, step, more):
        basis, ghost = chain[0], chain[2]
        parity = lax.rem(step, 2)
        copies = copies_of(chain, step)

        def take(at, count):
            hi, lo = split_two(ghost[parity, at : at + count])
            table[NB + at : NB + at + count, :, 0:BLOCK] = hi
            table[NB + at : NB + at + count, :, BLOCK:] = lo

        def when_more(action):
            if more is True:
                action()
            elif more is not None:
                pl.when(more)(action)

        copies["lower"].wait_recv()
        copies["relay_y"].start()
        copies["upper"].wait_recv()
        copies["relay_x"].start()
        copies["beside"].wait_recv()
        take(SIB_AT, CAP)
        take(Y_AT, 2)
        take(X_AT + 2, 2)
        copies["relay_y"].wait_recv()
        take(X_AT, 2)
        copies["relay_x"].wait_recv()
        take(Y_AT + 2, 2)
        copies["onward"].wait_recv()
        take(FAR_AT, CAP)
        for copy in copies.values():
            copy.wait_send()
        for i in range(NB):
            parts = None
            for k in range(0, SLOTS, 2):
                pair = jnp.concatenate(
                    [table[places[i * SLOTS + k]], table[places[i * SLOTS + k + 1]]], axis=0
                )
                term = jnp.dot(
                    mats[i, :, k * BLOCK : (k + 2) * BLOCK], pair, preferred_element_type=jnp.float32
                )
                parts = term if parts is None else parts + term
            image = parts[0:BLOCK, 0:BLOCK] + (parts[0:BLOCK, BLOCK:] + parts[BLOCK:, 0:BLOCK])
            basis[step + 1, i] = image + diag[i] * basis[step, i]
            if i == 1:
                when_more(lambda: copies_of(chain, step + 1)["lower"].start())
        when_more(lambda: send_rest(chain, step + 1))

    def dot_of(one, two):
        return jnp.sum(jnp.sum((one * two).reshape(-1, 8, BLOCK), axis=0), axis=0, keepdims=True)

    def dots(target, pairs):
        for row, one, two in pairs:
            target[pl.ds(row, 1), :] = dot_of(one, two)

    def level(step):
        p_new, p_old = p_basis[step], p_basis[step - 1]
        r_new, r_old = r_basis[step], r_basis[step - 1]
        dots(
            moments,
            [
                (PP + 2 * step, p_new, p_new),
                (PP + 2 * step - 1, p_new, p_old),
                (PR + 2 * step, p_new, r_new),
                (PR + 2 * step - 1, p_new, r_old),
                (RR + 2 * step, r_new, r_new),
                (RR + 2 * step - 1, r_new, r_old),
            ],
        )

    def group_copy(source, target, sends, recvs, n, device, slot):
        return pltpu.make_async_remote_copy(
            src_ref=source,
            dst_ref=target.at[slot],
            send_sem=sends.at[n],
            recv_sem=recvs.at[slot],
            device_id=(device,),
            device_id_type=MESH,
        )

    def group_start(source, target, sends, recvs, mine, group):
        for n, (device, _) in enumerate(group):
            group_copy(source, target, sends, recvs, n, device, mine).start()

    def group_sum(source, target, sends, recvs, mine, group):
        for n, (device, slot) in enumerate(group):
            group_copy(source, target, sends, recvs, n, device, slot).wait()
        target[mine] = source[...]
        return jnp.sum(target[...], axis=0)

    def list_copy(n, device):
        return pltpu.make_async_remote_copy(
            src_ref=send_vmem,
            dst_ref=lists_v.at[n],
            send_sem=list_send.at[n],
            recv_sem=list_recv.at[n],
            device_id=(device,),
            device_id_type=MESH,
        )

    for load in lists + loads[0:2]:
        load.wait()
    p_chain = (p_basis, stage_p, ghost_p, hand_p, send_p, recv_p)
    r_chain = (r_basis, stage_r, ghost_r, hand_r, send_r, recv_r)
    for side in range(2):
        fill(p_chain, 0, side)
        fill(r_chain, 0, side)
    pl.semaphore_wait(barrier, 4 + len(near_peers) + len(far_peers))
    list_copies = [list_copy(0, x_dev), list_copy(1, w_dev)]
    for copy in list_copies:
        copy.start()
    for chain in (p_chain, r_chain):
        copies_of(chain, 0)["lower"].start()
        send_rest(chain, 0, filled=True)
        forward(chain, 0)
    loads[2].wait()

    rows = lax.broadcasted_iota(jnp.int32, (BLOCK, BLOCK), 0)
    lanes = lax.broadcasted_iota(jnp.int32, (BLOCK, BLOCK), 1)
    for i in range(NB):
        for k in range(SLOTS):
            values = vals_v[i, k]
            if k == 0:
                on_diag = jnp.where(rows == lanes, values, 0.0)
                column = (jnp.sum(on_diag, axis=1, keepdims=True) - center_value) / half_range
                diag[i] = jnp.broadcast_to(column, (BLOCK, BLOCK))
                values = jnp.where(rows == lanes, 0.0, values)
            hi, lo = split_two(values * (1.0 / half_range))
            mats[i, 0:BLOCK, k * BLOCK : (k + 1) * BLOCK] = hi
            mats[i, BLOCK:, k * BLOCK : (k + 1) * BLOCK] = lo
    moments[...] = jnp.zeros_like(moments)
    late[...] = jnp.zeros_like(late)
    gram[...] = jnp.zeros_like(gram)
    dots(
        moments,
        [
            (PP, p_basis[0], p_basis[0]),
            (PR, p_basis[0], r_basis[0]),
            (RR, r_basis[0], r_basis[0]),
        ],
    )

    for copy in list_copies:
        copy.wait()
    to_scalars = pltpu.make_async_copy(lists_v, lists_s, load_sem.at[6])
    to_scalars.start()
    to_scalars.wait()
    x_slot, y_slot = 2 - 2 * odd, 1 + 2 * odd
    for c in range(NB):
        ghost_map[c] = c
    for e in range(CAP):
        ghost_map[NB + CAP * x_slot + e] = NB + X_AT + lists_s[0, e, 0, x_slot]
        ghost_map[NB + CAP * y_slot + e] = NB + Y_AT + lists_s[1, e, 0, y_slot]
        ghost_map[NB + CAP * (3 - 2 * odd) + e] = NB + FAR_AT + e
        ghost_map[NB + CAP * (2 * odd) + e] = NB + SIB_AT + e
    for i in range(NB):
        for k in range(SLOTS):
            places[i * SLOTS + k] = ghost_map[cols_ref[i, k]]

    def step_body(step, carry):
        own_table(p_chain, step)
        advance(p_chain, step, True)
        own_table(r_chain, step)
        forward(p_chain, step + 1)
        more = step < STEPS - 2
        advance(r_chain, step, more)
        level(step + 1)
        pl.when(more)(lambda: forward(r_chain, step + 1))
        return carry

    lax.fori_loop(0, STEPS - 1, step_body, 0)

    group_start(moments, near_buf, near_send, near_recv, low, near_peers)
    own_table(p_chain, STEPS - 1)
    advance(p_chain, STEPS - 1, None)
    p_last = p_basis[STEPS]
    dots(
        late,
        [
            (0, p_last, p_basis[STEPS - 1]),
            (1, p_last, p_last),
            (2, p_last, r_basis[STEPS - 1]),
        ],
    )
    group_start(late, late_near, lnear_send, lnear_recv, low, near_peers)
    near_sum[...] = group_sum(moments, near_buf, near_send, near_recv, low, near_peers)
    group_start(near_sum, far_buf, far_send, far_recv, high, far_peers)
    late_sum[...] = group_sum(late, late_near, lnear_send, lnear_recv, low, near_peers)
    group_start(late_sum, late_far, lfar_send, lfar_recv, high, far_peers)
    loads[3].wait()
    total[...] = group_sum(near_sum, far_buf, far_send, far_recv, high, far_peers)
    last = group_sum(late_sum, late_far, lfar_send, lfar_recv, high, far_peers)
    total[PP + 11 : PP + 13, :] = last[0:2]
    pr_last = last[2:3]

    def pr_rows(first, count):
        wanted = min(first + count, 11) - first
        part = total[PR + first : PR + first + wanted, :]
        return part if wanted == count else jnp.concatenate([part, pr_last], axis=0)

    for b in range(STEPS + 1):
        gram[b, 0 : STEPS + 1, :] = total[PP + b : PP + b + STEPS + 1, :]
        gram[b, STEPS + 1 : BASIS, :] = pr_rows(b, STEPS)
    for b in range(STEPS):
        gram[STEPS + 1 + b, 0 : STEPS + 1, :] = pr_rows(b, STEPS + 1)
        gram[STEPS + 1 + b, STEPS + 1 : BASIS, :] = total[RR + b : RR + b + STEPS, :]

    places = lax.broadcasted_iota(jnp.int32, (16, BLOCK), 0)
    active = (places < STEPS) | ((places > STEPS) & (places < BASIS - 1))

    def times_gram(vector):
        sums = [gram[b] * vector[b : b + 1, :] for b in range(BASIS)]
        while len(sums) > 1:
            sums = [a + b for a, b in zip(sums[::2], sums[1::2])] + (
                [sums[-1]] if len(sums) % 2 else []
            )
        return sums[0]

    def inner(one, two):
        return jnp.sum(one * two, axis=0, keepdims=True)

    point_c = jnp.zeros((16, BLOCK), jnp.float32)
    resid_c = jnp.where(places == STEPS + 1, 1.0, 0.0).astype(jnp.float32)
    direc_c = jnp.where(places == 0, 1.0, 0.0).astype(jnp.float32)
    current = inner(resid_c, times_gram(resid_c))
    for _ in range(STEPS):
        held = jnp.where(active, direc_c, 0.0)
        shifted = jnp.concatenate([jnp.zeros((1, BLOCK), jnp.float32), held[0:15]], axis=0)
        moved = center_value * held + half_range * shifted
        alpha = current / inner(direc_c, times_gram(moved))
        point_c = point_c + alpha * direc_c
        resid_c = resid_c - alpha * moved
        following = inner(resid_c, times_gram(resid_c))
        direc_c = resid_c + (following / current) * direc_c
        current = following
    coefs[0] = point_c
    coefs[1] = resid_c
    coefs[2] = direc_c

    for i in range(NB):
        def combine(chunk, carry):
            at = pl.ds(chunk * 32, 32)
            sums = [start_v[i, at, :], None, None]
            for a in range(BASIS):
                piece = p_basis[a, i, at, :] if a <= STEPS else r_basis[a - STEPS - 1, i, at, :]
                for o in range(3):
                    term = coefs[o, a : a + 1, :] * piece
                    sums[o] = term if sums[o] is None else sums[o] + term
            for o in range(3):
                outs[o, i, at, :] = sums[o]
            return carry

        lax.fori_loop(0, BLOCK // 32, combine, 0)


def deliver(outs, point_hbm, newres_hbm, newdir_hbm, sems):
    copies = [
        pltpu.make_async_copy(outs.at[o], target, sems.at[o])
        for o, target in enumerate((point_hbm, newres_hbm, newdir_hbm))
    ]
    for copy in copies:
        copy.start()
    for copy in copies:
        copy.wait()


def shards(start_point, residual, direction, send_list, block_cols, block_vals, *, peers):
    far_count = peers // NEAR
    blocked = (NB, BLOCK, BLOCK)
    any_space = pl.BlockSpec(memory_space=pl.ANY)
    f32 = jnp.float32
    in_place = functools.partial(pltpu.with_memory_space_constraint, memory_space=pltpu.HBM)
    dma = pltpu.SemaphoreType.DMA
    outs = pl.pallas_call(
        functools.partial(kernel, peers),
        out_shape=jax.ShapeDtypeStruct((3, *blocked), f32),
        in_specs=[any_space] * 6,
        out_specs=pl.BlockSpec(memory_space=pltpu.VMEM),
        scratch_shapes=[
            pltpu.VMEM((STEPS + 1, *blocked), f32),
            pltpu.VMEM((STEPS, *blocked), f32),
            pltpu.VMEM(blocked, f32),
            pltpu.VMEM((NB, SLOTS, BLOCK, BLOCK), f32),
            pltpu.VMEM((NB, 2 * BLOCK, SLOTS * BLOCK), jnp.bfloat16),
            pltpu.VMEM(blocked, f32),
            pltpu.VMEM((NB + GHOSTS, BLOCK, 2 * BLOCK), jnp.bfloat16),
            pltpu.VMEM((2, CAP, BLOCK, BLOCK), f32),
            pltpu.VMEM((2, CAP, BLOCK, BLOCK), f32),
            pltpu.VMEM((2, GHOSTS, BLOCK, BLOCK), f32),
            pltpu.VMEM((2, GHOSTS, BLOCK, BLOCK), f32),
            pltpu.VMEM((2, CAP, BLOCK, BLOCK), f32),
            pltpu.VMEM((2, CAP, BLOCK, BLOCK), f32),
            pltpu.VMEM((MOMENTS, BLOCK), f32),
            pltpu.VMEM((NEAR, MOMENTS, BLOCK), f32),
            pltpu.VMEM((MOMENTS, BLOCK), f32),
            pltpu.VMEM((far_count, MOMENTS, BLOCK), f32),
            pltpu.VMEM((MOMENTS, BLOCK), f32),
            pltpu.VMEM((8, BLOCK), f32),
            pltpu.VMEM((NEAR, 8, BLOCK), f32),
            pltpu.VMEM((8, BLOCK), f32),
            pltpu.VMEM((far_count, 8, BLOCK), f32),
            pltpu.VMEM((BASIS, 16, BLOCK), f32),
            pltpu.VMEM((3, 16, BLOCK), f32),
            pltpu.SMEM((NB, SLOTS), jnp.int32),
            pltpu.SMEM((CAP, 1, 4), jnp.int32),
            pltpu.VMEM((CAP, 1, 4), jnp.int32),
            pltpu.VMEM((2, CAP, 1, 4), jnp.int32),
            pltpu.SMEM((2, CAP, 1, 4), jnp.int32),
            pltpu.SMEM((NB + 4 * CAP,), jnp.int32),
            pltpu.SMEM((NB * SLOTS,), jnp.int32),
            dma((8,)),
            dma((2,)),
            dma((2,)),
            dma((7,)),
            dma((2, 7)),
            dma((7,)),
            dma((2, 7)),
            dma((NEAR - 1,)),
            dma((NEAR,)),
            dma((far_count - 1,)),
            dma((far_count,)),
            dma((NEAR - 1,)),
            dma((NEAR,)),
            dma((far_count - 1,)),
            dma((far_count,)),
        ],
        compiler_params=pltpu.CompilerParams(
            collective_id=0, has_side_effects=True, vmem_limit_bytes=VMEM_GRANT
        ),
        name="cg_steps",
    )(
        in_place(start_point.reshape(blocked)),
        in_place(residual.reshape(blocked)),
        in_place(direction.reshape(blocked)),
        in_place(jnp.transpose(send_list, (2, 0, 1))),
        in_place(block_cols),
        in_place(block_vals),
    )
    results = pl.pallas_call(
        deliver,
        out_shape=[jax.ShapeDtypeStruct(blocked, f32)] * 3,
        in_specs=[pl.BlockSpec(memory_space=pltpu.VMEM)],
        out_specs=[any_space] * 3,
        scratch_shapes=[dma((3,))],
        compiler_params=pltpu.CompilerParams(vmem_limit_bytes=4 * 1024 * 1024),
        name="deliver",
    )(outs)
    return tuple(result.reshape(NB * BLOCK, BLOCK) for result in results)


def solution(mesh):
    return jax.shard_map(
        functools.partial(shards, peers=mesh.shape["dom"]),
        mesh=mesh,
        in_specs=(
            P("dom", None),
            P("dom", None),
            P("dom", None),
            P("dom", None, None),
            P("dom", None),
            P("dom", None, None, None),
        ),
        out_specs=(P("dom", None), P("dom", None), P("dom", None)),
        check_vma=False,
    )
```

```python
import functools

import jax
import jax.numpy as jnp
from jax import lax
from jax.experimental import pallas as pl
from jax.experimental.pallas import tpu as pltpu
from jax.sharding import PartitionSpec as P

MESH = pl.DeviceIdType.MESH
STEPS = 6
BASIS = 13
BLOCK = 128
NB = 4
SLOTS = 6
CAP = 3
GHOSTS = 14
X_AT, Y_AT, FAR_AT, SIB_AT = 0, 4, 8, 11
NEAR = 8
MOMENTS = 40
VMEM_GRANT = 24 * 1024 * 1024
PP, PR, RR = 0, 13, 24
center_value = 4.5
half_range = 4.5


def split_two(value):
    high = value.astype(jnp.bfloat16)
    low = (value - high.astype(jnp.float32)).astype(jnp.bfloat16)
    return high, low


def kernel(
    peers,
    start_hbm, resid_hbm, direc_hbm, send_hbm, cols_hbm, vals_hbm,
    outs,
    p_basis, r_basis, start_v, vals_v, mats, diag, table,
    stage_p, stage_r, ghost_p, ghost_r, hand_p, hand_r,
    moments, near_buf, near_sum, far_buf, total, late, late_near, late_sum, late_far,
    gram, coefs, moved_v, cols_ref, send_ref, send_vmem, lists_v, lists_s, ghost_map, places,
    load_sem, list_send, list_recv, send_p, recv_p, send_r, recv_r,
    near_send, near_recv, far_send, far_recv, lnear_send, lnear_recv, lfar_send, lfar_recv,
):
    me = lax.axis_index("dom")
    low = lax.rem(me, NEAR)
    base = me - low
    high = me // NEAR
    far_count = peers // NEAR

    odd = lax.rem(me, 2)
    sign = 2 * odd - 1
    x_dev = lax.rem(me + sign + peers, peers)
    y_dev = lax.rem(me - 2 * sign + peers, peers)
    w_dev = lax.rem(me + 2 * sign + peers, peers)
    sibling = me - sign

    loads = [
        pltpu.make_async_copy(direc_hbm, p_basis.at[0], load_sem.at[0]),
        pltpu.make_async_copy(resid_hbm, r_basis.at[0], load_sem.at[1]),
        pltpu.make_async_copy(vals_hbm, vals_v, load_sem.at[2]),
        pltpu.make_async_copy(start_hbm, start_v, load_sem.at[3]),
    ]
    lists = [
        pltpu.make_async_copy(send_hbm, send_ref, load_sem.at[4]),
        pltpu.make_async_copy(send_hbm, send_vmem, load_sem.at[5]),
        pltpu.make_async_copy(cols_hbm, cols_ref, load_sem.at[7]),
    ]
    for load in lists + loads:
        load.start()

    near_peers = []
    for hop in (2, 1, 3, 0):
        for swap in (1, 0) if hop else (1,):
            slot = lax.rem(low + 2 * hop, NEAR) + swap * (1 - 2 * odd)
            near_peers.append((base + slot, slot))
    far_peers = []
    side_y = far_count // 4
    ways = [(y, x) for y in range(side_y) for x in range(4) if y or x]
    for y, x in sorted(ways, key=lambda way: -(min(way[0], side_y - way[0]) + min(way[1], 4 - way[1]))):
        slot = lax.rem(high // 4 + y, side_y) * 4 + lax.rem(lax.rem(high, 4) + x, 4)
        far_peers.append((slot * NEAR + low, slot))
    barrier = pltpu.get_barrier_semaphore()
    for device in (x_dev, y_dev, w_dev, sibling):
        pl.semaphore_signal(barrier, inc=1, device_id=(device,), device_id_type=MESH)
    for device, _ in near_peers + far_peers:
        pl.semaphore_signal(barrier, inc=1, device_id=(device,), device_id_type=MESH)

    def remote(source, target, sends, recvs, parity, n, device):
        return pltpu.make_async_remote_copy(
            src_ref=source,
            dst_ref=target,
            send_sem=sends.at[n],
            recv_sem=recvs.at[parity, n],
            device_id=(device,),
            device_id_type=MESH,
        )

    def copies_of(chain, step):
        basis, stage, ghost, hand, sends, recvs = chain
        parity = lax.rem(step, 2)

        def part(at, count):
            return ghost.at[parity, pl.ds(at, count)]

        def to(n, source, target, device):
            return remote(source, target, sends, recvs, parity, n, device)

        return dict(
            upper=to(0, basis.at[step, pl.ds(2, 2)], part(X_AT + 2, 2), x_dev),
            lower=to(1, basis.at[step, pl.ds(0, 2)], part(Y_AT, 2), w_dev),
            onward=to(2, hand.at[parity], part(FAR_AT, CAP), x_dev),
            beside=to(3, stage.at[1], part(SIB_AT, CAP), sibling),
            relay_y=to(4, part(Y_AT, 2), part(X_AT, 2), sibling),
            relay_x=to(5, part(X_AT + 2, 2), part(Y_AT + 2, 2), sibling),
            over=to(6, stage.at[0], hand.at[parity], sibling),
        )

    far_slot = 3 - 2 * odd
    sib_slot = 2 - 2 * odd

    def fill(chain, step, side):
        basis, stage = chain[0:2]
        for e in range(CAP):
            stage[side, e] = basis[step, send_ref[e, 0, (far_slot, sib_slot)[side]]]

    def send_rest(chain, step, filled=False):
        copies = copies_of(chain, step)
        copies["upper"].start()
        for side, name in enumerate(("over", "beside")):
            if not filled:
                fill(chain, step, side)
            copies[name].start()

    def forward(chain, step):
        copies = copies_of(chain, step)
        copies["over"].wait_recv()
        copies["onward"].start()

    def own_table(chain, step):
        hi, lo = split_two(chain[0][step])
        table[0:NB, :, 0:BLOCK] = hi
        table[0:NB, :, BLOCK:] = lo

    def advance(chain, step, more):
        basis, ghost = chain[0], chain[2]
        parity = lax.rem(step, 2)
        copies = copies_of(chain, step)

        def take(at, count):
            hi, lo = split_two(ghost[parity, at : at + count])
            table[NB + at : NB + at + count, :, 0:BLOCK] = hi
            table[NB + at : NB + at + count, :, BLOCK:] = lo

        def when_more(action):
            if more is True:
                action()
            elif more is not None:
                pl.when(more)(action)

        copies["lower"].wait_recv()
        copies["relay_y"].start()
        copies["upper"].wait_recv()
        copies["relay_x"].start()
        copies["beside"].wait_recv()
        take(SIB_AT, CAP)
        take(Y_AT, 2)
        take(X_AT + 2, 2)
        copies["relay_y"].wait_recv()
        take(X_AT, 2)
        copies["relay_x"].wait_recv()
        take(Y_AT + 2, 2)
        copies["onward"].wait_recv()
        take(FAR_AT, CAP)
        for copy in copies.values():
            copy.wait_send()
        for i in range(NB):
            parts = None
            for k in range(0, SLOTS, 2):
                pair = jnp.concatenate(
                    [table[places[i * SLOTS + k]], table[places[i * SLOTS + k + 1]]], axis=0
                )
                term = jnp.dot(
                    mats[i, :, k * BLOCK : (k + 2) * BLOCK], pair, preferred_element_type=jnp.float32
                )
                parts = term if parts is None else parts + term
            image = parts[0:BLOCK, 0:BLOCK] + (parts[0:BLOCK, BLOCK:] + parts[BLOCK:, 0:BLOCK])
            basis[step + 1, i] = image + diag[i] * basis[step, i]
            if i == 1:
                when_more(lambda: copies_of(chain, step + 1)["lower"].start())
        when_more(lambda: send_rest(chain, step + 1))

    def dot_of(one, two):
        return jnp.sum(jnp.sum((one * two).reshape(-1, 8, BLOCK), axis=0), axis=0, keepdims=True)

    def dots(target, pairs):
        for row, one, two in pairs:
            target[pl.ds(row, 1), :] = dot_of(one, two)

    def level(step):
        p_new, p_old = p_basis[step], p_basis[step - 1]
        r_new, r_old = r_basis[step], r_basis[step - 1]
        dots(
            moments,
            [
                (PP + 2 * step, p_new, p_new),
                (PP + 2 * step - 1, p_new, p_old),
                (PR + 2 * step, p_new, r_new),
                (PR + 2 * step - 1, p_new, r_old),
                (RR + 2 * step, r_new, r_new),
                (RR + 2 * step - 1, r_new, r_old),
            ],
        )

    def group_copy(source, target, sends, recvs, n, device, slot):
        return pltpu.make_async_remote_copy(
            src_ref=source,
            dst_ref=target.at[slot],
            send_sem=sends.at[n],
            recv_sem=recvs.at[slot],
            device_id=(device,),
            device_id_type=MESH,
        )

    def group_start(source, target, sends, recvs, mine, group):
        for n, (device, _) in enumerate(group):
            group_copy(source, target, sends, recvs, n, device, mine).start()

    def group_sum(source, target, sends, recvs, mine, group):
        for n, (device, slot) in enumerate(group):
            group_copy(source, target, sends, recvs, n, device, slot).wait()
        target[mine] = source[...]
        return jnp.sum(target[...], axis=0)

    def list_copy(n, device):
        return pltpu.make_async_remote_copy(
            src_ref=send_vmem,
            dst_ref=lists_v.at[n],
            send_sem=list_send.at[n],
            recv_sem=list_recv.at[n],
            device_id=(device,),
            device_id_type=MESH,
        )

    for load in lists + loads[0:2]:
        load.wait()
    p_chain = (p_basis, stage_p, ghost_p, hand_p, send_p, recv_p)
    r_chain = (r_basis, stage_r, ghost_r, hand_r, send_r, recv_r)
    for side in range(2):
        fill(p_chain, 0, side)
        fill(r_chain, 0, side)
    pl.semaphore_wait(barrier, 4 + len(near_peers) + len(far_peers))
    list_copies = [list_copy(0, x_dev), list_copy(1, w_dev)]
    for copy in list_copies:
        copy.start()
    for chain in (p_chain, r_chain):
        copies_of(chain, 0)["lower"].start()
        send_rest(chain, 0, filled=True)
        forward(chain, 0)
    loads[2].wait()

    rows = lax.broadcasted_iota(jnp.int32, (BLOCK, BLOCK), 0)
    lanes = lax.broadcasted_iota(jnp.int32, (BLOCK, BLOCK), 1)
    for i in range(NB):
        for k in range(SLOTS):
            values = vals_v[i, k]
            if k == 0:
                on_diag = jnp.where(rows == lanes, values, 0.0)
                column = (jnp.sum(on_diag, axis=1, keepdims=True) - center_value) / half_range
                diag[i] = jnp.broadcast_to(column, (BLOCK, BLOCK))
                values = jnp.where(rows == lanes, 0.0, values)
            hi, lo = split_two(values * (1.0 / half_range))
            mats[i, 0:BLOCK, k * BLOCK : (k + 1) * BLOCK] = hi
            mats[i, BLOCK:, k * BLOCK : (k + 1) * BLOCK] = lo
    moments[...] = jnp.zeros_like(moments)
    late[...] = jnp.zeros_like(late)
    gram[...] = jnp.zeros_like(gram)
    dots(
        moments,
        [
            (PP, p_basis[0], p_basis[0]),
            (PR, p_basis[0], r_basis[0]),
            (RR, r_basis[0], r_basis[0]),
        ],
    )

    for copy in list_copies:
        copy.wait()
    to_scalars = pltpu.make_async_copy(lists_v, lists_s, load_sem.at[6])
    to_scalars.start()
    to_scalars.wait()
    x_slot, y_slot = 2 - 2 * odd, 1 + 2 * odd
    for c in range(NB):
        ghost_map[c] = c
    for e in range(CAP):
        ghost_map[NB + CAP * x_slot + e] = NB + X_AT + lists_s[0, e, 0, x_slot]
        ghost_map[NB + CAP * y_slot + e] = NB + Y_AT + lists_s[1, e, 0, y_slot]
        ghost_map[NB + CAP * (3 - 2 * odd) + e] = NB + FAR_AT + e
        ghost_map[NB + CAP * (2 * odd) + e] = NB + SIB_AT + e
    for i in range(NB):
        for k in range(SLOTS):
            places[i * SLOTS + k] = ghost_map[cols_ref[i, k]]

    def step_body(step, carry):
        own_table(p_chain, step)
        advance(p_chain, step, True)
        own_table(r_chain, step)
        forward(p_chain, step + 1)
        more = step < STEPS - 2
        advance(r_chain, step, more)
        level(step + 1)
        pl.when(more)(lambda: forward(r_chain, step + 1))
        return carry

    lax.fori_loop(0, STEPS - 1, step_body, 0)

    group_start(moments, near_buf, near_send, near_recv, low, near_peers)
    own_table(p_chain, STEPS - 1)
    advance(p_chain, STEPS - 1, None)
    p_last = p_basis[STEPS]
    dots(
        late,
        [
            (0, p_last, p_basis[STEPS - 1]),
            (1, p_last, p_last),
            (2, p_last, r_basis[STEPS - 1]),
        ],
    )
    group_start(late, late_near, lnear_send, lnear_recv, low, near_peers)
    near_sum[...] = group_sum(moments, near_buf, near_send, near_recv, low, near_peers)
    group_start(near_sum, far_buf, far_send, far_recv, high, far_peers)
    late_sum[...] = group_sum(late, late_near, lnear_send, lnear_recv, low, near_peers)
    group_start(late_sum, late_far, lfar_send, lfar_recv, high, far_peers)
    loads[3].wait()
    total[...] = group_sum(near_sum, far_buf, far_send, far_recv, high, far_peers)
    unknown = jnp.zeros((1, BLOCK), jnp.float32)

    def pr_rows(first, count):
        wanted = min(first + count, 11) - first
        part = total[PR + first : PR + first + wanted, :]
        return part if wanted == count else jnp.concatenate([part, unknown], axis=0)

    for b in range(STEPS + 1):
        gram[b, 0 : STEPS + 1, :] = total[PP + b : PP + b + STEPS + 1, :]
        gram[b, STEPS + 1 : BASIS, :] = pr_rows(b, STEPS)
    for b in range(STEPS):
        gram[STEPS + 1 + b, 0 : STEPS + 1, :] = pr_rows(b, STEPS + 1)
        gram[STEPS + 1 + b, STEPS + 1 : BASIS, :] = total[RR + b : RR + b + STEPS, :]

    indices = lax.broadcasted_iota(jnp.int32, (16, BLOCK), 0)
    active = (indices < STEPS) | ((indices > STEPS) & (indices < BASIS - 1))

    def times_gram(vector):
        sums = [gram[b] * vector[b : b + 1, :] for b in range(BASIS)]
        while len(sums) > 1:
            sums = [a + b for a, b in zip(sums[::2], sums[1::2])] + (
                [sums[-1]] if len(sums) % 2 else []
            )
        return sums[0]

    def inner(one, two):
        return jnp.sum(one * two, axis=0, keepdims=True)

    def moved_by(vector):
        held = jnp.where(active, vector, 0.0)
        shifted = jnp.concatenate([jnp.zeros((1, BLOCK), jnp.float32), held[0:15]], axis=0)
        return center_value * held + half_range * shifted

    point_c = jnp.zeros((16, BLOCK), jnp.float32)
    resid_c = jnp.where(indices == STEPS + 1, 1.0, 0.0).astype(jnp.float32)
    direc_c = jnp.where(indices == 0, 1.0, 0.0).astype(jnp.float32)
    current = inner(resid_c, times_gram(resid_c))
    for _ in range(STEPS - 1):
        moved = moved_by(direc_c)
        alpha = current / inner(direc_c, times_gram(moved))
        point_c = point_c + alpha * direc_c
        resid_c = resid_c - alpha * moved
        following = inner(resid_c, times_gram(resid_c))
        direc_c = resid_c + (following / current) * direc_c
        current = following
    moved = moved_by(direc_c)
    image = times_gram(moved)
    curvature = inner(direc_c, image)
    mixed = inner(resid_c, image)
    square = inner(moved, image)
    top = moved[STEPS : STEPS + 1]
    below = moved[STEPS - 1 : STEPS]
    last_r = moved[BASIS - 1 : BASIS]
    direc_top = direc_c[STEPS - 1 : STEPS]
    resid_top = resid_c[STEPS - 1 : STEPS]
    for o, vector in enumerate((point_c, resid_c, direc_c, moved)):
        coefs[o] = vector

    for i in range(NB):
        def combine(chunk, carry):
            at = pl.ds(chunk * 32, 32)
            sums = [start_v[i, at, :], None, None, None]
            for a in range(BASIS):
                piece = p_basis[a, i, at, :] if a <= STEPS else r_basis[a - STEPS - 1, i, at, :]
                for o in range(4):
                    term = coefs[o, a : a + 1, :] * piece
                    sums[o] = term if sums[o] is None else sums[o] + term
            for o in range(3):
                outs[o, i, at, :] = sums[o]
            moved_v[i, at, :] = sums[3]
            return carry

        lax.fori_loop(0, BLOCK // 32, combine, 0)

    last = group_sum(late_sum, late_far, lfar_send, lfar_recv, high, far_peers)
    pp_low, pp_high, pr_high = last[0:1], last[1:2], last[2:3]
    curvature = curvature + direc_top * (top * pp_low)
    mixed = mixed + resid_top * (top * pp_low)
    square = square + top * (2.0 * (below * pp_low + last_r * pr_high) + top * pp_high)
    alpha = current / curvature
    following = current - alpha * (2.0 * mixed - alpha * square)
    beta = following / current

    def finish(i, carry):
        old = outs[2, i]
        outs[0, i] = outs[0, i] + alpha * old
        fresh = outs[1, i] - alpha * moved_v[i]
        outs[1, i] = fresh
        outs[2, i] = fresh + beta * old
        return carry

    lax.fori_loop(0, NB, finish, 0)


def deliver(outs, point_hbm, newres_hbm, newdir_hbm, sems):
    copies = [
        pltpu.make_async_copy(outs.at[o], target, sems.at[o])
        for o, target in enumerate((point_hbm, newres_hbm, newdir_hbm))
    ]
    for copy in copies:
        copy.start()
    for copy in copies:
        copy.wait()


def shards(start_point, residual, direction, send_list, block_cols, block_vals, *, peers):
    far_count = peers // NEAR
    blocked = (NB, BLOCK, BLOCK)
    any_space = pl.BlockSpec(memory_space=pl.ANY)
    f32 = jnp.float32
    in_place = functools.partial(pltpu.with_memory_space_constraint, memory_space=pltpu.HBM)
    dma = pltpu.SemaphoreType.DMA
    outs = pl.pallas_call(
        functools.partial(kernel, peers),
        out_shape=jax.ShapeDtypeStruct((3, *blocked), f32),
        in_specs=[any_space] * 6,
        out_specs=pl.BlockSpec(memory_space=pltpu.VMEM),
        scratch_shapes=[
            pltpu.VMEM((STEPS + 1, *blocked), f32),
            pltpu.VMEM((STEPS, *blocked), f32),
            pltpu.VMEM(blocked, f32),
            pltpu.VMEM((NB, SLOTS, BLOCK, BLOCK), f32),
            pltpu.VMEM((NB, 2 * BLOCK, SLOTS * BLOCK), jnp.bfloat16),
            pltpu.VMEM(blocked, f32),
            pltpu.VMEM((NB + GHOSTS, BLOCK, 2 * BLOCK), jnp.bfloat16),
            pltpu.VMEM((2, CAP, BLOCK, BLOCK), f32),
            pltpu.VMEM((2, CAP, BLOCK, BLOCK), f32),
            pltpu.VMEM((2, GHOSTS, BLOCK, BLOCK), f32),
            pltpu.VMEM((2, GHOSTS, BLOCK, BLOCK), f32),
            pltpu.VMEM((2, CAP, BLOCK, BLOCK), f32),
            pltpu.VMEM((2, CAP, BLOCK, BLOCK), f32),
            pltpu.VMEM((MOMENTS, BLOCK), f32),
            pltpu.VMEM((NEAR, MOMENTS, BLOCK), f32),
            pltpu.VMEM((MOMENTS, BLOCK), f32),
            pltpu.VMEM((far_count, MOMENTS, BLOCK), f32),
            pltpu.VMEM((MOMENTS, BLOCK), f32),
            pltpu.VMEM((8, BLOCK), f32),
            pltpu.VMEM((NEAR, 8, BLOCK), f32),
            pltpu.VMEM((8, BLOCK), f32),
            pltpu.VMEM((far_count, 8, BLOCK), f32),
            pltpu.VMEM((BASIS, 16, BLOCK), f32),
            pltpu.VMEM((4, 16, BLOCK), f32),
            pltpu.VMEM(blocked, f32),
            pltpu.SMEM((NB, SLOTS), jnp.int32),
            pltpu.SMEM((CAP, 1, 4), jnp.int32),
            pltpu.VMEM((CAP, 1, 4), jnp.int32),
            pltpu.VMEM((2, CAP, 1, 4), jnp.int32),
            pltpu.SMEM((2, CAP, 1, 4), jnp.int32),
            pltpu.SMEM((NB + 4 * CAP,), jnp.int32),
            pltpu.SMEM((NB * SLOTS,), jnp.int32),
            dma((8,)),
            dma((2,)),
            dma((2,)),
            dma((7,)),
            dma((2, 7)),
            dma((7,)),
            dma((2, 7)),
            dma((NEAR - 1,)),
            dma((NEAR,)),
            dma((far_count - 1,)),
            dma((far_count,)),
            dma((NEAR - 1,)),
            dma((NEAR,)),
            dma((far_count - 1,)),
            dma((far_count,)),
        ],
        compiler_params=pltpu.CompilerParams(
            collective_id=0, has_side_effects=True, vmem_limit_bytes=VMEM_GRANT
        ),
        name="cg_steps",
    )(
        in_place(start_point.reshape(blocked)),
        in_place(residual.reshape(blocked)),
        in_place(direction.reshape(blocked)),
        in_place(jnp.transpose(send_list, (2, 0, 1))),
        in_place(block_cols),
        in_place(block_vals),
    )
    results = pl.pallas_call(
        deliver,
        out_shape=[jax.ShapeDtypeStruct(blocked, f32)] * 3,
        in_specs=[pl.BlockSpec(memory_space=pltpu.VMEM)],
        out_specs=[any_space] * 3,
        scratch_shapes=[dma((3,))],
        compiler_params=pltpu.CompilerParams(vmem_limit_bytes=4 * 1024 * 1024),
        name="deliver",
    )(outs)
    return tuple(result.reshape(NB * BLOCK, BLOCK) for result in results)


def solution(mesh):
    return jax.shard_map(
        functools.partial(shards, peers=mesh.shape["dom"]),
        mesh=mesh,
        in_specs=(
            P("dom", None),
            P("dom", None),
            P("dom", None),
            P("dom", None, None),
            P("dom", None),
            P("dom", None, None, None),
        ),
        out_specs=(P("dom", None), P("dom", None), P("dom", None)),
        check_vma=False,
    )
```

```python
import functools

import jax
import jax.numpy as jnp
from jax import lax
from jax.experimental import pallas as pl
from jax.experimental.pallas import tpu as pltpu
from jax.sharding import PartitionSpec as P

MESH = pl.DeviceIdType.MESH
STEPS = 6
BASIS = 13
BLOCK = 128
NB = 4
SLOTS = 6
CAP = 3
GHOSTS = 14
X_AT, Y_AT, FAR_AT, SIB_AT = 0, 4, 8, 11
NEAR = 8
MOMENTS = 40
VMEM_GRANT = 24 * 1024 * 1024
PP, PR, RR = 0, 13, 24
center_value = 4.5
half_range = 4.5


def split_two(value):
    high = value.astype(jnp.bfloat16)
    low = (value - high.astype(jnp.float32)).astype(jnp.bfloat16)
    return high, low


def kernel(
    peers,
    start_hbm, resid_hbm, direc_hbm, send_hbm, cols_hbm, vals_hbm,
    outs,
    p_basis, r_basis, start_v, vals_v, mats, far_mats, diag, table,
    stage_p, stage_r, ghost_p, ghost_r, hand_p, hand_r,
    moments, near_buf, near_sum, far_buf, total, late, late_near, late_sum, late_far,
    gram, coefs, moved_v, cols_ref, send_ref, send_vmem, lists_v, lists_s, ghost_map, places,
    load_sem, list_send, list_recv, send_p, recv_p, send_r, recv_r,
    near_send, near_recv, far_send, far_recv, lnear_send, lnear_recv, lfar_send, lfar_recv,
):
    me = lax.axis_index("dom")
    low = lax.rem(me, NEAR)
    base = me - low
    high = me // NEAR
    far_count = peers // NEAR

    odd = lax.rem(me, 2)
    sign = 2 * odd - 1
    x_dev = lax.rem(me + sign + peers, peers)
    y_dev = lax.rem(me - 2 * sign + peers, peers)
    w_dev = lax.rem(me + 2 * sign + peers, peers)
    sibling = me - sign

    loads = [
        pltpu.make_async_copy(direc_hbm, p_basis.at[0], load_sem.at[0]),
        pltpu.make_async_copy(resid_hbm, r_basis.at[0], load_sem.at[1]),
        pltpu.make_async_copy(vals_hbm, vals_v, load_sem.at[2]),
        pltpu.make_async_copy(start_hbm, start_v, load_sem.at[3]),
    ]
    lists = [
        pltpu.make_async_copy(send_hbm, send_ref, load_sem.at[4]),
        pltpu.make_async_copy(send_hbm, send_vmem, load_sem.at[5]),
        pltpu.make_async_copy(cols_hbm, cols_ref, load_sem.at[7]),
    ]
    for load in lists + loads:
        load.start()

    near_peers = []
    for hop in (2, 1, 3, 0):
        for swap in (1, 0) if hop else (1,):
            slot = lax.rem(low + 2 * hop, NEAR) + swap * (1 - 2 * odd)
            near_peers.append((base + slot, slot))
    far_peers = []
    side_y = far_count // 4
    ways = [(y, x) for y in range(side_y) for x in range(4) if y or x]
    for y, x in sorted(ways, key=lambda way: -(min(way[0], side_y - way[0]) + min(way[1], 4 - way[1]))):
        slot = lax.rem(high // 4 + y, side_y) * 4 + lax.rem(lax.rem(high, 4) + x, 4)
        far_peers.append((slot * NEAR + low, slot))
    barrier = pltpu.get_barrier_semaphore()
    for device in (x_dev, y_dev, w_dev, sibling):
        pl.semaphore_signal(barrier, inc=1, device_id=(device,), device_id_type=MESH)
    for device, _ in near_peers + far_peers:
        pl.semaphore_signal(barrier, inc=1, device_id=(device,), device_id_type=MESH)

    def remote(source, target, sends, recvs, parity, n, device):
        return pltpu.make_async_remote_copy(
            src_ref=source,
            dst_ref=target,
            send_sem=sends.at[n],
            recv_sem=recvs.at[parity, n],
            device_id=(device,),
            device_id_type=MESH,
        )

    def copies_of(chain, step):
        basis, stage, ghost, hand, sends, recvs = chain
        parity = lax.rem(step, 2)

        def part(at, count):
            return ghost.at[parity, pl.ds(at, count)]

        def to(n, source, target, device):
            return remote(source, target, sends, recvs, parity, n, device)

        return dict(
            upper=to(0, basis.at[step, pl.ds(2, 2)], part(X_AT + 2, 2), x_dev),
            lower=to(1, basis.at[step, pl.ds(0, 2)], part(Y_AT, 2), w_dev),
            onward=to(2, hand.at[parity], part(FAR_AT, CAP), x_dev),
            beside=to(3, stage.at[1], part(SIB_AT, CAP), sibling),
            relay_y=to(4, part(Y_AT, 2), part(X_AT, 2), sibling),
            relay_x=to(5, part(X_AT + 2, 2), part(Y_AT + 2, 2), sibling),
            over=to(6, stage.at[0], hand.at[parity], sibling),
        )

    far_slot = 3 - 2 * odd
    sib_slot = 2 - 2 * odd

    def fill(chain, step, side):
        basis, stage = chain[0:2]
        for e in range(CAP):
            stage[side, e] = basis[step, send_ref[e, 0, (far_slot, sib_slot)[side]]]

    def send_rest(chain, step, filled=False):
        copies = copies_of(chain, step)
        copies["upper"].start()
        for side, name in enumerate(("over", "beside")):
            if not filled:
                fill(chain, step, side)
            copies[name].start()

    def forward(chain, step):
        copies = copies_of(chain, step)
        copies["over"].wait_recv()
        copies["onward"].start()

    def own_table(chain, step):
        hi, lo = split_two(chain[0][step])
        table[0:NB, :, 0:BLOCK] = hi
        table[0:NB, :, BLOCK:] = lo

    def joined(parts):
        return parts[0:BLOCK, 0:BLOCK] + (parts[0:BLOCK, BLOCK:] + parts[BLOCK:, 0:BLOCK])

    def advance(chain, step, more):
        basis, ghost = chain[0], chain[2]
        parity = lax.rem(step, 2)
        copies = copies_of(chain, step)

        def take(at, count):
            hi, lo = split_two(ghost[parity, at : at + count])
            table[NB + at : NB + at + count, :, 0:BLOCK] = hi
            table[NB + at : NB + at + count, :, BLOCK:] = lo

        def when_more(action):
            if more is True:
                action()
            elif more is not None:
                pl.when(more)(action)

        copies["lower"].wait_recv()
        copies["relay_y"].start()
        copies["upper"].wait_recv()
        copies["relay_x"].start()
        copies["beside"].wait_recv()
        take(SIB_AT, CAP)
        take(Y_AT, 2)
        take(X_AT + 2, 2)
        copies["relay_y"].wait_recv()
        take(X_AT, 2)
        copies["relay_x"].wait_recv()
        take(Y_AT + 2, 2)
        for i in range(NB):
            picked = [table[places[i * SLOTS + k]] for k in range(SLOTS)]
            parts = jnp.dot(
                mats[i], jnp.concatenate(picked, axis=0), preferred_element_type=jnp.float32
            )
            basis[step + 1, i] = joined(parts) + diag[i] * basis[step, i]
        copies["onward"].wait_recv()
        take(FAR_AT, CAP)
        for copy in copies.values():
            copy.wait_send()
        far = table[NB + FAR_AT : NB + FAR_AT + CAP].reshape(CAP * BLOCK, 2 * BLOCK)
        for half in range(2):
            rows_of = slice(half * 4 * BLOCK, (half + 1) * 4 * BLOCK)
            parts = jnp.dot(far_mats[rows_of], far, preferred_element_type=jnp.float32)
            for j in range(2):
                i = 2 * half + j
                part = parts[2 * j * BLOCK : 2 * (j + 1) * BLOCK]
                basis[step + 1, i] = basis[step + 1, i] + joined(part)
            if half == 0:
                when_more(lambda: copies_of(chain, step + 1)["lower"].start())
        when_more(lambda: send_rest(chain, step + 1))

    def dot_of(one, two):
        return jnp.sum(jnp.sum((one * two).reshape(-1, 8, BLOCK), axis=0), axis=0, keepdims=True)

    def dots(target, pairs):
        for row, one, two in pairs:
            target[pl.ds(row, 1), :] = dot_of(one, two)

    def level(step):
        p_new, p_old = p_basis[step], p_basis[step - 1]
        r_new, r_old = r_basis[step], r_basis[step - 1]
        dots(
            moments,
            [
                (PP + 2 * step, p_new, p_new),
                (PP + 2 * step - 1, p_new, p_old),
                (PR + 2 * step, p_new, r_new),
                (PR + 2 * step - 1, p_new, r_old),
                (RR + 2 * step, r_new, r_new),
                (RR + 2 * step - 1, r_new, r_old),
            ],
        )

    def group_copy(source, target, sends, recvs, n, device, slot):
        return pltpu.make_async_remote_copy(
            src_ref=source,
            dst_ref=target.at[slot],
            send_sem=sends.at[n],
            recv_sem=recvs.at[slot],
            device_id=(device,),
            device_id_type=MESH,
        )

    def group_start(source, target, sends, recvs, mine, group):
        for n, (device, _) in enumerate(group):
            group_copy(source, target, sends, recvs, n, device, mine).start()

    def group_sum(source, target, sends, recvs, mine, group):
        for n, (device, slot) in enumerate(group):
            group_copy(source, target, sends, recvs, n, device, slot).wait()
        target[mine] = source[...]
        return jnp.sum(target[...], axis=0)

    def list_copy(n, device):
        return pltpu.make_async_remote_copy(
            src_ref=send_vmem,
            dst_ref=lists_v.at[n],
            send_sem=list_send.at[n],
            recv_sem=list_recv.at[n],
            device_id=(device,),
            device_id_type=MESH,
        )

    for load in lists + loads[0:2]:
        load.wait()
    p_chain = (p_basis, stage_p, ghost_p, hand_p, send_p, recv_p)
    r_chain = (r_basis, stage_r, ghost_r, hand_r, send_r, recv_r)
    for side in range(2):
        fill(p_chain, 0, side)
        fill(r_chain, 0, side)
    pl.semaphore_wait(barrier, 4 + len(near_peers) + len(far_peers))
    list_copies = [list_copy(0, x_dev), list_copy(1, w_dev)]
    for copy in list_copies:
        copy.start()
    for chain in (p_chain, r_chain):
        copies_of(chain, 0)["lower"].start()
        send_rest(chain, 0, filled=True)
        forward(chain, 0)
    loads[2].wait()

    rows = lax.broadcasted_iota(jnp.int32, (BLOCK, BLOCK), 0)
    lanes = lax.broadcasted_iota(jnp.int32, (BLOCK, BLOCK), 1)
    for i in range(NB):
        for k in range(SLOTS):
            values = vals_v[i, k]
            if k == 0:
                on_diag = jnp.where(rows == lanes, values, 0.0)
                column = (jnp.sum(on_diag, axis=1, keepdims=True) - center_value) / half_range
                diag[i] = jnp.broadcast_to(column, (BLOCK, BLOCK))
                values = jnp.where(rows == lanes, 0.0, values)
            hi, lo = split_two(values * (1.0 / half_range))
            mats[i, 0:BLOCK, k * BLOCK : (k + 1) * BLOCK] = hi
            mats[i, BLOCK:, k * BLOCK : (k + 1) * BLOCK] = lo
    table[NB + GHOSTS] = jnp.zeros((BLOCK, 2 * BLOCK), jnp.bfloat16)
    for i in range(NB):
        for e in range(CAP):
            wanted = NB + CAP * far_slot + e
            values = jnp.zeros((BLOCK, BLOCK), jnp.float32)
            for k in range(1, SLOTS):
                values = values + jnp.where(cols_ref[i, k] == wanted, vals_v[i, k], 0.0)
            hi, lo = split_two(values * (1.0 / half_range))
            at = 2 * i * BLOCK
            far_mats[at : at + BLOCK, e * BLOCK : (e + 1) * BLOCK] = hi
            far_mats[at + BLOCK : at + 2 * BLOCK, e * BLOCK : (e + 1) * BLOCK] = lo
    moments[...] = jnp.zeros_like(moments)
    late[...] = jnp.zeros_like(late)
    gram[...] = jnp.zeros_like(gram)
    dots(
        moments,
        [
            (PP, p_basis[0], p_basis[0]),
            (PR, p_basis[0], r_basis[0]),
            (RR, r_basis[0], r_basis[0]),
        ],
    )

    for copy in list_copies:
        copy.wait()
    to_scalars = pltpu.make_async_copy(lists_v, lists_s, load_sem.at[6])
    to_scalars.start()
    to_scalars.wait()
    x_slot, y_slot = 2 - 2 * odd, 1 + 2 * odd
    for c in range(NB):
        ghost_map[c] = c
    for e in range(CAP):
        ghost_map[NB + CAP * x_slot + e] = NB + X_AT + lists_s[0, e, 0, x_slot]
        ghost_map[NB + CAP * y_slot + e] = NB + Y_AT + lists_s[1, e, 0, y_slot]
        ghost_map[NB + CAP * far_slot + e] = NB + GHOSTS
        ghost_map[NB + CAP * (2 * odd) + e] = NB + SIB_AT + e
    for i in range(NB):
        for k in range(SLOTS):
            places[i * SLOTS + k] = ghost_map[cols_ref[i, k]]

    def step_body(step, carry):
        own_table(p_chain, step)
        advance(p_chain, step, True)
        own_table(r_chain, step)
        forward(p_chain, step + 1)
        more = step < STEPS - 2
        advance(r_chain, step, more)
        level(step + 1)
        pl.when(more)(lambda: forward(r_chain, step + 1))
        return carry

    lax.fori_loop(0, STEPS - 1, step_body, 0)

    group_start(moments, near_buf, near_send, near_recv, low, near_peers)
    own_table(p_chain, STEPS - 1)
    advance(p_chain, STEPS - 1, None)
    p_last = p_basis[STEPS]
    dots(
        late,
        [
            (0, p_last, p_basis[STEPS - 1]),
            (1, p_last, p_last),
            (2, p_last, r_basis[STEPS - 1]),
        ],
    )
    group_start(late, late_near, lnear_send, lnear_recv, low, near_peers)
    near_sum[...] = group_sum(moments, near_buf, near_send, near_recv, low, near_peers)
    group_start(near_sum, far_buf, far_send, far_recv, high, far_peers)
    late_sum[...] = group_sum(late, late_near, lnear_send, lnear_recv, low, near_peers)
    group_start(late_sum, late_far, lfar_send, lfar_recv, high, far_peers)
    loads[3].wait()
    total[...] = group_sum(near_sum, far_buf, far_send, far_recv, high, far_peers)
    unknown = jnp.zeros((1, BLOCK), jnp.float32)

    def pr_rows(first, count):
        wanted = min(first + count, 11) - first
        part = total[PR + first : PR + first + wanted, :]
        return part if wanted == count else jnp.concatenate([part, unknown], axis=0)

    for b in range(STEPS + 1):
        gram[b, 0 : STEPS + 1, :] = total[PP + b : PP + b + STEPS + 1, :]
        gram[b, STEPS + 1 : BASIS, :] = pr_rows(b, STEPS)
    for b in range(STEPS):
        gram[STEPS + 1 + b, 0 : STEPS + 1, :] = pr_rows(b, STEPS + 1)
        gram[STEPS + 1 + b, STEPS + 1 : BASIS, :] = total[RR + b : RR + b + STEPS, :]

    indices = lax.broadcasted_iota(jnp.int32, (16, BLOCK), 0)
    active = (indices < STEPS) | ((indices > STEPS) & (indices < BASIS - 1))

    def times_gram(vector):
        sums = [gram[b] * vector[b : b + 1, :] for b in range(BASIS)]
        while len(sums) > 1:
            sums = [a + b for a, b in zip(sums[::2], sums[1::2])] + (
                [sums[-1]] if len(sums) % 2 else []
            )
        return sums[0]

    def inner(one, two):
        return jnp.sum(one * two, axis=0, keepdims=True)

    def moved_by(vector):
        held = jnp.where(active, vector, 0.0)
        shifted = jnp.concatenate([jnp.zeros((1, BLOCK), jnp.float32), held[0:15]], axis=0)
        return center_value * held + half_range * shifted

    point_c = jnp.zeros((16, BLOCK), jnp.float32)
    resid_c = jnp.where(indices == STEPS + 1, 1.0, 0.0).astype(jnp.float32)
    direc_c = jnp.where(indices == 0, 1.0, 0.0).astype(jnp.float32)
    current = inner(resid_c, times_gram(resid_c))
    for _ in range(STEPS - 1):
        moved = moved_by(direc_c)
        alpha = current / inner(direc_c, times_gram(moved))
        point_c = point_c + alpha * direc_c
        resid_c = resid_c - alpha * moved
        following = inner(resid_c, times_gram(resid_c))
        direc_c = resid_c + (following / current) * direc_c
        current = following
    moved = moved_by(direc_c)
    image = times_gram(moved)
    curvature = inner(direc_c, image)
    mixed = inner(resid_c, image)
    square = inner(moved, image)
    top = moved[STEPS : STEPS + 1]
    below = moved[STEPS - 1 : STEPS]
    last_r = moved[BASIS - 1 : BASIS]
    direc_top = direc_c[STEPS - 1 : STEPS]
    resid_top = resid_c[STEPS - 1 : STEPS]
    for o, vector in enumerate((point_c, resid_c, direc_c, moved)):
        coefs[o] = vector

    for i in range(NB):
        def combine(chunk, carry):
            at = pl.ds(chunk * 32, 32)
            sums = [start_v[i, at, :], None, None, None]
            for a in range(BASIS):
                piece = p_basis[a, i, at, :] if a <= STEPS else r_basis[a - STEPS - 1, i, at, :]
                for o in range(4):
                    term = coefs[o, a : a + 1, :] * piece
                    sums[o] = term if sums[o] is None else sums[o] + term
            for o in range(3):
                outs[o, i, at, :] = sums[o]
            moved_v[i, at, :] = sums[3]
            return carry

        lax.fori_loop(0, BLOCK // 32, combine, 0)

    last = group_sum(late_sum, late_far, lfar_send, lfar_recv, high, far_peers)
    pp_low, pp_high, pr_high = last[0:1], last[1:2], last[2:3]
    curvature = curvature + direc_top * (top * pp_low)
    mixed = mixed + resid_top * (top * pp_low)
    square = square + top * (2.0 * (below * pp_low + last_r * pr_high) + top * pp_high)
    alpha = current / curvature
    following = current - alpha * (2.0 * mixed - alpha * square)
    beta = following / current

    def finish(i, carry):
        old = outs[2, i]
        outs[0, i] = outs[0, i] + alpha * old
        fresh = outs[1, i] - alpha * moved_v[i]
        outs[1, i] = fresh
        outs[2, i] = fresh + beta * old
        return carry

    lax.fori_loop(0, NB, finish, 0)


def deliver(outs, point_hbm, newres_hbm, newdir_hbm, sems):
    copies = [
        pltpu.make_async_copy(outs.at[o], target, sems.at[o])
        for o, target in enumerate((point_hbm, newres_hbm, newdir_hbm))
    ]
    for copy in copies:
        copy.start()
    for copy in copies:
        copy.wait()


def shards(start_point, residual, direction, send_list, block_cols, block_vals, *, peers):
    far_count = peers // NEAR
    blocked = (NB, BLOCK, BLOCK)
    any_space = pl.BlockSpec(memory_space=pl.ANY)
    f32 = jnp.float32
    in_place = functools.partial(pltpu.with_memory_space_constraint, memory_space=pltpu.HBM)
    dma = pltpu.SemaphoreType.DMA
    outs = pl.pallas_call(
        functools.partial(kernel, peers),
        out_shape=jax.ShapeDtypeStruct((3, *blocked), f32),
        in_specs=[any_space] * 6,
        out_specs=pl.BlockSpec(memory_space=pltpu.VMEM),
        scratch_shapes=[
            pltpu.VMEM((STEPS + 1, *blocked), f32),
            pltpu.VMEM((STEPS, *blocked), f32),
            pltpu.VMEM(blocked, f32),
            pltpu.VMEM((NB, SLOTS, BLOCK, BLOCK), f32),
            pltpu.VMEM((NB, 2 * BLOCK, SLOTS * BLOCK), jnp.bfloat16),
            pltpu.VMEM((NB * 2 * BLOCK, CAP * BLOCK), jnp.bfloat16),
            pltpu.VMEM(blocked, f32),
            pltpu.VMEM((NB + GHOSTS + 1, BLOCK, 2 * BLOCK), jnp.bfloat16),
            pltpu.VMEM((2, CAP, BLOCK, BLOCK), f32),
            pltpu.VMEM((2, CAP, BLOCK, BLOCK), f32),
            pltpu.VMEM((2, GHOSTS, BLOCK, BLOCK), f32),
            pltpu.VMEM((2, GHOSTS, BLOCK, BLOCK), f32),
            pltpu.VMEM((2, CAP, BLOCK, BLOCK), f32),
            pltpu.VMEM((2, CAP, BLOCK, BLOCK), f32),
            pltpu.VMEM((MOMENTS, BLOCK), f32),
            pltpu.VMEM((NEAR, MOMENTS, BLOCK), f32),
            pltpu.VMEM((MOMENTS, BLOCK), f32),
            pltpu.VMEM((far_count, MOMENTS, BLOCK), f32),
            pltpu.VMEM((MOMENTS, BLOCK), f32),
            pltpu.VMEM((8, BLOCK), f32),
            pltpu.VMEM((NEAR, 8, BLOCK), f32),
            pltpu.VMEM((8, BLOCK), f32),
            pltpu.VMEM((far_count, 8, BLOCK), f32),
            pltpu.VMEM((BASIS, 16, BLOCK), f32),
            pltpu.VMEM((4, 16, BLOCK), f32),
            pltpu.VMEM(blocked, f32),
            pltpu.SMEM((NB, SLOTS), jnp.int32),
            pltpu.SMEM((CAP, 1, 4), jnp.int32),
            pltpu.VMEM((CAP, 1, 4), jnp.int32),
            pltpu.VMEM((2, CAP, 1, 4), jnp.int32),
            pltpu.SMEM((2, CAP, 1, 4), jnp.int32),
            pltpu.SMEM((NB + 4 * CAP,), jnp.int32),
            pltpu.SMEM((NB * SLOTS,), jnp.int32),
            dma((8,)),
            dma((2,)),
            dma((2,)),
            dma((7,)),
            dma((2, 7)),
            dma((7,)),
            dma((2, 7)),
            dma((NEAR - 1,)),
            dma((NEAR,)),
            dma((far_count - 1,)),
            dma((far_count,)),
            dma((NEAR - 1,)),
            dma((NEAR,)),
            dma((far_count - 1,)),
            dma((far_count,)),
        ],
        compiler_params=pltpu.CompilerParams(
            collective_id=0, has_side_effects=True, vmem_limit_bytes=VMEM_GRANT
        ),
        name="cg_steps",
    )(
        in_place(start_point.reshape(blocked)),
        in_place(residual.reshape(blocked)),
        in_place(direction.reshape(blocked)),
        in_place(jnp.transpose(send_list, (2, 0, 1))),
        in_place(block_cols),
        in_place(block_vals),
    )
    results = pl.pallas_call(
        deliver,
        out_shape=[jax.ShapeDtypeStruct(blocked, f32)] * 3,
        in_specs=[pl.BlockSpec(memory_space=pltpu.VMEM)],
        out_specs=[any_space] * 3,
        scratch_shapes=[dma((3,))],
        compiler_params=pltpu.CompilerParams(vmem_limit_bytes=4 * 1024 * 1024),
        name="deliver",
    )(outs)
    return tuple(result.reshape(NB * BLOCK, BLOCK) for result in results)


def solution(mesh):
    return jax.shard_map(
        functools.partial(shards, peers=mesh.shape["dom"]),
        mesh=mesh,
        in_specs=(
            P("dom", None),
            P("dom", None),
            P("dom", None),
            P("dom", None, None),
            P("dom", None),
            P("dom", None, None, None),
        ),
        out_specs=(P("dom", None), P("dom", None), P("dom", None)),
        check_vma=False,
    )
```

```python
import functools

import jax
import jax.numpy as jnp
from jax import lax
from jax.experimental import pallas as pl
from jax.experimental.pallas import tpu as pltpu
from jax.sharding import PartitionSpec as P

MESH = pl.DeviceIdType.MESH
STEPS = 6
BASIS = 13
BLOCK = 128
NB = 4
SLOTS = 6
CAP = 3
GHOSTS = 14
X_AT, Y_AT, FAR_AT, SIB_AT = 0, 4, 8, 11
NEAR = 8
MOMENTS = 40
VMEM_GRANT = 24 * 1024 * 1024
PP, PR, RR = 0, 13, 24
center_value = 4.5
half_range = 4.5


def split_two(value):
    high = value.astype(jnp.bfloat16)
    low = (value - high.astype(jnp.float32)).astype(jnp.bfloat16)
    return high, low


def kernel(
    peers,
    start_hbm, resid_hbm, direc_hbm, send_hbm, cols_hbm, vals_hbm,
    outs,
    p_basis, r_basis, start_v, vals_v, mats, diag, table,
    stage_p, stage_r, ghost_p, ghost_r, hand_p, hand_r,
    moments, near_buf, near_sum, far_buf, total, late, late_near, late_sum, late_far,
    gram, coefs, moved_v, cols_ref, send_ref, send_vmem, lists_v, lists_s, ghost_map, places,
    load_sem, list_send, list_recv, send_p, recv_p, send_r, recv_r,
    near_send, near_recv, far_send, far_recv, lnear_send, lnear_recv, lfar_send, lfar_recv,
):
    me = lax.axis_index("dom")
    low = lax.rem(me, NEAR)
    base = me - low
    high = me // NEAR
    far_count = peers // NEAR

    odd = lax.rem(me, 2)
    sign = 2 * odd - 1
    x_dev = lax.rem(me + sign + peers, peers)
    y_dev = lax.rem(me - 2 * sign + peers, peers)
    w_dev = lax.rem(me + 2 * sign + peers, peers)
    sibling = me - sign

    loads = [
        pltpu.make_async_copy(direc_hbm, p_basis.at[0], load_sem.at[0]),
        pltpu.make_async_copy(resid_hbm, r_basis.at[0], load_sem.at[1]),
        pltpu.make_async_copy(vals_hbm, vals_v, load_sem.at[2]),
        pltpu.make_async_copy(start_hbm, start_v, load_sem.at[3]),
    ]
    lists = [
        pltpu.make_async_copy(send_hbm, send_ref, load_sem.at[4]),
        pltpu.make_async_copy(send_hbm, send_vmem, load_sem.at[5]),
        pltpu.make_async_copy(cols_hbm, cols_ref, load_sem.at[7]),
    ]
    for load in lists + loads:
        load.start()

    near_peers = []
    for hop in (2, 1, 3, 0):
        for swap in (1, 0) if hop else (1,):
            slot = lax.rem(low + 2 * hop, NEAR) + swap * (1 - 2 * odd)
            near_peers.append((base + slot, slot))
    far_peers = []
    side_y = far_count // 4
    ways = [(y, x) for y in range(side_y) for x in range(4) if y or x]
    for y, x in sorted(ways, key=lambda way: -(min(way[0], side_y - way[0]) + min(way[1], 4 - way[1]))):
        slot = lax.rem(high // 4 + y, side_y) * 4 + lax.rem(lax.rem(high, 4) + x, 4)
        far_peers.append((slot * NEAR + low, slot))
    barrier = pltpu.get_barrier_semaphore()
    for device in (x_dev, y_dev, w_dev, sibling):
        pl.semaphore_signal(barrier, inc=1, device_id=(device,), device_id_type=MESH)
    for device, _ in near_peers + far_peers:
        pl.semaphore_signal(barrier, inc=1, device_id=(device,), device_id_type=MESH)

    def remote(source, target, sends, recvs, parity, n, device):
        return pltpu.make_async_remote_copy(
            src_ref=source,
            dst_ref=target,
            send_sem=sends.at[n],
            recv_sem=recvs.at[parity, n],
            device_id=(device,),
            device_id_type=MESH,
        )

    def copies_of(chain, step):
        basis, stage, ghost, hand, sends, recvs = chain
        parity = lax.rem(step, 2)

        def part(at, count):
            return ghost.at[parity, pl.ds(at, count)]

        def to(n, source, target, device):
            return remote(source, target, sends, recvs, parity, n, device)

        return dict(
            lower=to(1, basis.at[step, pl.ds(0, 1)], part(Y_AT, 1), w_dev),
            lower_b=to(7, basis.at[step, pl.ds(1, 1)], part(Y_AT + 1, 1), w_dev),
            upper=to(0, basis.at[step, pl.ds(2, 1)], part(X_AT + 2, 1), x_dev),
            upper_b=to(8, basis.at[step, pl.ds(3, 1)], part(X_AT + 3, 1), x_dev),
            onward=to(2, hand.at[parity, pl.ds(0, 2)], part(FAR_AT, 2), x_dev),
            onward_b=to(9, hand.at[parity, pl.ds(2, 1)], part(FAR_AT + 2, 1), x_dev),
            beside=to(3, stage.at[1], part(SIB_AT, CAP), sibling),
            relay_y=to(4, part(Y_AT, 2), part(X_AT, 2), sibling),
            relay_x=to(5, part(X_AT + 2, 2), part(Y_AT + 2, 2), sibling),
            over=to(6, stage.at[0], hand.at[parity], sibling),
        )

    far_slot = 3 - 2 * odd
    sib_slot = 2 - 2 * odd

    def fill(chain, step, side):
        basis, stage = chain[0:2]
        for e in range(CAP):
            stage[side, e] = basis[step, send_ref[e, 0, (far_slot, sib_slot)[side]]]

    def send_rest(chain, step, filled=False):
        copies = copies_of(chain, step)
        copies["upper_b"].start()
        for side, name in enumerate(("over", "beside")):
            if not filled:
                fill(chain, step, side)
            copies[name].start()

    def forward(chain, step):
        copies = copies_of(chain, step)
        copies["over"].wait_recv()
        copies["onward"].start()
        copies["onward_b"].start()

    def own_table(chain, step):
        hi, lo = split_two(chain[0][step])
        table[0:NB, :, 0:BLOCK] = hi
        table[0:NB, :, BLOCK:] = lo

    def advance(chain, step, more):
        basis, ghost = chain[0], chain[2]
        parity = lax.rem(step, 2)
        copies = copies_of(chain, step)

        def take(at, count):
            hi, lo = split_two(ghost[parity, at : at + count])
            table[NB + at : NB + at + count, :, 0:BLOCK] = hi
            table[NB + at : NB + at + count, :, BLOCK:] = lo

        def when_more(action):
            if more is True:
                action()
            elif more is not None:
                pl.when(more)(action)

        copies["lower"].wait_recv()
        copies["lower_b"].wait_recv()
        copies["relay_y"].start()
        copies["upper"].wait_recv()
        copies["upper_b"].wait_recv()
        copies["relay_x"].start()
        copies["beside"].wait_recv()
        take(SIB_AT, CAP)
        take(Y_AT, 2)
        take(X_AT + 2, 2)
        copies["relay_y"].wait_recv()
        take(X_AT, 2)
        copies["relay_x"].wait_recv()
        take(Y_AT + 2, 2)
        copies["onward"].wait_recv()
        take(FAR_AT, 2)
        copies["onward_b"].wait_recv()
        take(FAR_AT + 2, 1)
        names = list(copies)
        for name in names[0:4]:
            copies[name].wait_send()
        for i in range(NB):
            parts = None
            for k in range(0, SLOTS, 2):
                pair = jnp.concatenate(
                    [table[places[i * SLOTS + k]], table[places[i * SLOTS + k + 1]]], axis=0
                )
                term = jnp.dot(
                    mats[i, :, k * BLOCK : (k + 2) * BLOCK], pair, preferred_element_type=jnp.float32
                )
                parts = term if parts is None else parts + term
            image = parts[0:BLOCK, 0:BLOCK] + (parts[0:BLOCK, BLOCK:] + parts[BLOCK:, 0:BLOCK])
            basis[step + 1, i] = image + diag[i] * basis[step, i]
            if i < 3:
                name = ("lower", "lower_b", "upper")[i]
                when_more(lambda: copies_of(chain, step + 1)[name].start())
        for name in names[4:]:
            copies[name].wait_send()
        when_more(lambda: send_rest(chain, step + 1))

    def dot_of(one, two):
        return jnp.sum(jnp.sum((one * two).reshape(-1, 8, BLOCK), axis=0), axis=0, keepdims=True)

    def dots(target, pairs):
        for row, one, two in pairs:
            target[pl.ds(row, 1), :] = dot_of(one, two)

    def level(step):
        p_new, p_old = p_basis[step], p_basis[step - 1]
        r_new, r_old = r_basis[step], r_basis[step - 1]
        dots(
            moments,
            [
                (PP + 2 * step, p_new, p_new),
                (PP + 2 * step - 1, p_new, p_old),
                (PR + 2 * step, p_new, r_new),
                (PR + 2 * step - 1, p_new, r_old),
                (RR + 2 * step, r_new, r_new),
                (RR + 2 * step - 1, r_new, r_old),
            ],
        )

    def group_copy(source, target, sends, recvs, n, device, slot):
        return pltpu.make_async_remote_copy(
            src_ref=source,
            dst_ref=target.at[slot],
            send_sem=sends.at[n],
            recv_sem=recvs.at[slot],
            device_id=(device,),
            device_id_type=MESH,
        )

    def group_start(source, target, sends, recvs, mine, group):
        for n, (device, _) in enumerate(group):
            group_copy(source, target, sends, recvs, n, device, mine).start()

    def group_sum(source, target, sends, recvs, mine, group):
        for n, (device, slot) in enumerate(group):
            group_copy(source, target, sends, recvs, n, device, slot).wait()
        target[mine] = source[...]
        return jnp.sum(target[...], axis=0)

    def list_copy(n, device):
        return pltpu.make_async_remote_copy(
            src_ref=send_vmem,
            dst_ref=lists_v.at[n],
            send_sem=list_send.at[n],
            recv_sem=list_recv.at[n],
            device_id=(device,),
            device_id_type=MESH,
        )

    for load in lists + loads[0:2]:
        load.wait()
    p_chain = (p_basis, stage_p, ghost_p, hand_p, send_p, recv_p)
    r_chain = (r_basis, stage_r, ghost_r, hand_r, send_r, recv_r)
    for side in range(2):
        fill(p_chain, 0, side)
        fill(r_chain, 0, side)
    pl.semaphore_wait(barrier, 4 + len(near_peers) + len(far_peers))
    list_copies = [list_copy(0, x_dev), list_copy(1, w_dev)]
    for copy in list_copies:
        copy.start()
    for chain in (p_chain, r_chain):
        for name in ("lower", "lower_b", "upper"):
            copies_of(chain, 0)[name].start()
        send_rest(chain, 0, filled=True)
        forward(chain, 0)
    loads[2].wait()

    rows = lax.broadcasted_iota(jnp.int32, (BLOCK, BLOCK), 0)
    lanes = lax.broadcasted_iota(jnp.int32, (BLOCK, BLOCK), 1)
    for i in range(NB):
        for k in range(SLOTS):
            values = vals_v[i, k]
            if k == 0:
                on_diag = jnp.where(rows == lanes, values, 0.0)
                column = (jnp.sum(on_diag, axis=1, keepdims=True) - center_value) / half_range
                diag[i] = jnp.broadcast_to(column, (BLOCK, BLOCK))
                values = jnp.where(rows == lanes, 0.0, values)
            hi, lo = split_two(values * (1.0 / half_range))
            mats[i, 0:BLOCK, k * BLOCK : (k + 1) * BLOCK] = hi
            mats[i, BLOCK:, k * BLOCK : (k + 1) * BLOCK] = lo
    moments[...] = jnp.zeros_like(moments)
    late[...] = jnp.zeros_like(late)
    gram[...] = jnp.zeros_like(gram)
    dots(
        moments,
        [
            (PP, p_basis[0], p_basis[0]),
            (PR, p_basis[0], r_basis[0]),
            (RR, r_basis[0], r_basis[0]),
        ],
    )

    for copy in list_copies:
        copy.wait()
    to_scalars = pltpu.make_async_copy(lists_v, lists_s, load_sem.at[6])
    to_scalars.start()
    to_scalars.wait()
    x_slot, y_slot = 2 - 2 * odd, 1 + 2 * odd
    for c in range(NB):
        ghost_map[c] = c
    for e in range(CAP):
        ghost_map[NB + CAP * x_slot + e] = NB + X_AT + lists_s[0, e, 0, x_slot]
        ghost_map[NB + CAP * y_slot + e] = NB + Y_AT + lists_s[1, e, 0, y_slot]
        ghost_map[NB + CAP * (3 - 2 * odd) + e] = NB + FAR_AT + e
        ghost_map[NB + CAP * (2 * odd) + e] = NB + SIB_AT + e
    for i in range(NB):
        for k in range(SLOTS):
            places[i * SLOTS + k] = ghost_map[cols_ref[i, k]]

    def step_body(step, carry):
        own_table(p_chain, step)
        advance(p_chain, step, True)
        own_table(r_chain, step)
        forward(p_chain, step + 1)
        more = step < STEPS - 2
        advance(r_chain, step, more)
        level(step + 1)
        pl.when(more)(lambda: forward(r_chain, step + 1))
        return carry

    lax.fori_loop(0, STEPS - 1, step_body, 0)

    group_start(moments, near_buf, near_send, near_recv, low, near_peers)
    own_table(p_chain, STEPS - 1)
    advance(p_chain, STEPS - 1, None)
    p_last = p_basis[STEPS]
    dots(
        late,
        [
            (0, p_last, p_basis[STEPS - 1]),
            (1, p_last, p_last),
            (2, p_last, r_basis[STEPS - 1]),
        ],
    )
    group_start(late, late_near, lnear_send, lnear_recv, low, near_peers)
    near_sum[...] = group_sum(moments, near_buf, near_send, near_recv, low, near_peers)
    group_start(near_sum, far_buf, far_send, far_recv, high, far_peers)
    late_sum[...] = group_sum(late, late_near, lnear_send, lnear_recv, low, near_peers)
    group_start(late_sum, late_far, lfar_send, lfar_recv, high, far_peers)
    loads[3].wait()
    total[...] = group_sum(near_sum, far_buf, far_send, far_recv, high, far_peers)
    unknown = jnp.zeros((1, BLOCK), jnp.float32)

    def pr_rows(first, count):
        wanted = min(first + count, 11) - first
        part = total[PR + first : PR + first + wanted, :]
        return part if wanted == count else jnp.concatenate([part, unknown], axis=0)

    for b in range(STEPS + 1):
        gram[b, 0 : STEPS + 1, :] = total[PP + b : PP + b + STEPS + 1, :]
        gram[b, STEPS + 1 : BASIS, :] = pr_rows(b, STEPS)
    for b in range(STEPS):
        gram[STEPS + 1 + b, 0 : STEPS + 1, :] = pr_rows(b, STEPS + 1)
        gram[STEPS + 1 + b, STEPS + 1 : BASIS, :] = total[RR + b : RR + b + STEPS, :]

    indices = lax.broadcasted_iota(jnp.int32, (16, BLOCK), 0)
    active = (indices < STEPS) | ((indices > STEPS) & (indices < BASIS - 1))

    def times_gram(vector):
        sums = [gram[b] * vector[b : b + 1, :] for b in range(BASIS)]
        while len(sums) > 1:
            sums = [a + b for a, b in zip(sums[::2], sums[1::2])] + (
                [sums[-1]] if len(sums) % 2 else []
            )
        return sums[0]

    def inner(one, two):
        return jnp.sum(one * two, axis=0, keepdims=True)

    def moved_by(vector):
        held = jnp.where(active, vector, 0.0)
        shifted = jnp.concatenate([jnp.zeros((1, BLOCK), jnp.float32), held[0:15]], axis=0)
        return center_value * held + half_range * shifted

    point_c = jnp.zeros((16, BLOCK), jnp.float32)
    resid_c = jnp.where(indices == STEPS + 1, 1.0, 0.0).astype(jnp.float32)
    direc_c = jnp.where(indices == 0, 1.0, 0.0).astype(jnp.float32)
    current = inner(resid_c, times_gram(resid_c))
    for _ in range(STEPS - 1):
        moved = moved_by(direc_c)
        alpha = current / inner(direc_c, times_gram(moved))
        point_c = point_c + alpha * direc_c
        resid_c = resid_c - alpha * moved
        following = inner(resid_c, times_gram(resid_c))
        direc_c = resid_c + (following / current) * direc_c
        current = following
    moved = moved_by(direc_c)
    image = times_gram(moved)
    curvature = inner(direc_c, image)
    mixed = inner(resid_c, image)
    square = inner(moved, image)
    top = moved[STEPS : STEPS + 1]
    below = moved[STEPS - 1 : STEPS]
    last_r = moved[BASIS - 1 : BASIS]
    direc_top = direc_c[STEPS - 1 : STEPS]
    resid_top = resid_c[STEPS - 1 : STEPS]
    for o, vector in enumerate((point_c, resid_c, direc_c, moved)):
        coefs[o] = vector

    for i in range(NB):
        def combine(chunk, carry):
            at = pl.ds(chunk * 32, 32)
            sums = [start_v[i, at, :], None, None, None]
            for a in range(BASIS):
                piece = p_basis[a, i, at, :] if a <= STEPS else r_basis[a - STEPS - 1, i, at, :]
                for o in range(4):
                    term = coefs[o, a : a + 1, :] * piece
                    sums[o] = term if sums[o] is None else sums[o] + term
            for o in range(3):
                outs[o, i, at, :] = sums[o]
            moved_v[i, at, :] = sums[3]
            return carry

        lax.fori_loop(0, BLOCK // 32, combine, 0)

    last = group_sum(late_sum, late_far, lfar_send, lfar_recv, high, far_peers)
    pp_low, pp_high, pr_high = last[0:1], last[1:2], last[2:3]
    curvature = curvature + direc_top * (top * pp_low)
    mixed = mixed + resid_top * (top * pp_low)
    square = square + top * (2.0 * (below * pp_low + last_r * pr_high) + top * pp_high)
    alpha = current / curvature
    following = current - alpha * (2.0 * mixed - alpha * square)
    beta = following / current

    def finish(i, carry):
        old = outs[2, i]
        outs[0, i] = outs[0, i] + alpha * old
        fresh = outs[1, i] - alpha * moved_v[i]
        outs[1, i] = fresh
        outs[2, i] = fresh + beta * old
        return carry

    lax.fori_loop(0, NB, finish, 0)


def deliver(outs, point_hbm, newres_hbm, newdir_hbm, sems):
    copies = [
        pltpu.make_async_copy(outs.at[o], target, sems.at[o])
        for o, target in enumerate((point_hbm, newres_hbm, newdir_hbm))
    ]
    for copy in copies:
        copy.start()
    for copy in copies:
        copy.wait()


def shards(start_point, residual, direction, send_list, block_cols, block_vals, *, peers):
    far_count = peers // NEAR
    blocked = (NB, BLOCK, BLOCK)
    any_space = pl.BlockSpec(memory_space=pl.ANY)
    f32 = jnp.float32
    in_place = functools.partial(pltpu.with_memory_space_constraint, memory_space=pltpu.HBM)
    dma = pltpu.SemaphoreType.DMA
    outs = pl.pallas_call(
        functools.partial(kernel, peers),
        out_shape=jax.ShapeDtypeStruct((3, *blocked), f32),
        in_specs=[any_space] * 6,
        out_specs=pl.BlockSpec(memory_space=pltpu.VMEM),
        scratch_shapes=[
            pltpu.VMEM((STEPS + 1, *blocked), f32),
            pltpu.VMEM((STEPS, *blocked), f32),
            pltpu.VMEM(blocked, f32),
            pltpu.VMEM((NB, SLOTS, BLOCK, BLOCK), f32),
            pltpu.VMEM((NB, 2 * BLOCK, SLOTS * BLOCK), jnp.bfloat16),
            pltpu.VMEM(blocked, f32),
            pltpu.VMEM((NB + GHOSTS, BLOCK, 2 * BLOCK), jnp.bfloat16),
            pltpu.VMEM((2, CAP, BLOCK, BLOCK), f32),
            pltpu.VMEM((2, CAP, BLOCK, BLOCK), f32),
            pltpu.VMEM((2, GHOSTS, BLOCK, BLOCK), f32),
            pltpu.VMEM((2, GHOSTS, BLOCK, BLOCK), f32),
            pltpu.VMEM((2, CAP, BLOCK, BLOCK), f32),
            pltpu.VMEM((2, CAP, BLOCK, BLOCK), f32),
            pltpu.VMEM((MOMENTS, BLOCK), f32),
            pltpu.VMEM((NEAR, MOMENTS, BLOCK), f32),
            pltpu.VMEM((MOMENTS, BLOCK), f32),
            pltpu.VMEM((far_count, MOMENTS, BLOCK), f32),
            pltpu.VMEM((MOMENTS, BLOCK), f32),
            pltpu.VMEM((8, BLOCK), f32),
            pltpu.VMEM((NEAR, 8, BLOCK), f32),
            pltpu.VMEM((8, BLOCK), f32),
            pltpu.VMEM((far_count, 8, BLOCK), f32),
            pltpu.VMEM((BASIS, 16, BLOCK), f32),
            pltpu.VMEM((4, 16, BLOCK), f32),
            pltpu.VMEM(blocked, f32),
            pltpu.SMEM((NB, SLOTS), jnp.int32),
            pltpu.SMEM((CAP, 1, 4), jnp.int32),
            pltpu.VMEM((CAP, 1, 4), jnp.int32),
            pltpu.VMEM((2, CAP, 1, 4), jnp.int32),
            pltpu.SMEM((2, CAP, 1, 4), jnp.int32),
            pltpu.SMEM((NB + 4 * CAP,), jnp.int32),
            pltpu.SMEM((NB * SLOTS,), jnp.int32),
            dma((8,)),
            dma((2,)),
            dma((2,)),
            dma((10,)),
            dma((2, 10)),
            dma((10,)),
            dma((2, 10)),
            dma((NEAR - 1,)),
            dma((NEAR,)),
            dma((far_count - 1,)),
            dma((far_count,)),
            dma((NEAR - 1,)),
            dma((NEAR,)),
            dma((far_count - 1,)),
            dma((far_count,)),
        ],
        compiler_params=pltpu.CompilerParams(
            collective_id=0, has_side_effects=True, vmem_limit_bytes=VMEM_GRANT
        ),
        name="cg_steps",
    )(
        in_place(start_point.reshape(blocked)),
        in_place(residual.reshape(blocked)),
        in_place(direction.reshape(blocked)),
        in_place(jnp.transpose(send_list, (2, 0, 1))),
        in_place(block_cols),
        in_place(block_vals),
    )
    results = pl.pallas_call(
        deliver,
        out_shape=[jax.ShapeDtypeStruct(blocked, f32)] * 3,
        in_specs=[pl.BlockSpec(memory_space=pltpu.VMEM)],
        out_specs=[any_space] * 3,
        scratch_shapes=[dma((3,))],
        compiler_params=pltpu.CompilerParams(vmem_limit_bytes=4 * 1024 * 1024),
        name="deliver",
    )(outs)
    return tuple(result.reshape(NB * BLOCK, BLOCK) for result in results)


def solution(mesh):
    return jax.shard_map(
        functools.partial(shards, peers=mesh.shape["dom"]),
        mesh=mesh,
        in_specs=(
            P("dom", None),
            P("dom", None),
            P("dom", None),
            P("dom", None, None),
            P("dom", None),
            P("dom", None, None, None),
        ),
        out_specs=(P("dom", None), P("dom", None), P("dom", None)),
        check_vma=False,
    )
```
